128 devices in a mesh: dp: 4 (over y), cp: 32 (over x, z, core).
Axes of the slice: x: 4, y: 4, z: 4, core: 2. Of those that a mesh axis runs over, the one named last changes fastest.
Arguments:
- hidden: bfloat16 [4, 4096, 2880], P('dp', 'cp'), may hold values from -8 to 8
- norm_gain: float32 [2880], replicated, may hold values from 0.5 to 1.5
- query_weight: bfloat16 [2880, 2048], replicated, may hold values from -4 to 4
- keyval_weight: bfloat16 [2880, 512], replicated, may hold values from -1 to 1
- sink_logits: float32 [32], replicated, may hold values from -1 to 3
- document_ids: int32 [4, 4096], P('dp', 'cp'), may hold values from 0 to 15, never falling along the last dimension, each value on 1 to 1024 neighbouring positions
- block_owner: int32 [4, 32, 32], P('dp', 'cp'), may hold values from 0 to 31, each once within a row
- loss_mask: int32 [4, 4096], P('dp', 'cp'), may hold values from 0 to 1, as said below
Outputs:
- attended: bfloat16 [4, 4096, 2048], P('dp', 'cp')
- row_lse: float32 [4, 32, 4096], P('dp', None, 'cp')
- token_weight: float32 [4, 4096], P('dp', 'cp')
The draws below stay inside these ranges and needn't reach their ends.
Inputs may be any that keep to these rules, and one draw needn't show every extreme that they name: `document_ids`: in each group the ids start at 0, never fall, rise by at most one from a position to the next and end at 15; a document holds at most 1024 positions. `block_owner`: for each group and device the row of 32 entries is a permutation of 0 to 31. `loss_mask`: the last flag of each group is 1.
All inputs are finite; a program needn't handle non-finite values.
Results may differ from the reference program's by a relative error of at most 0.008.
Values may be sent and summed in bfloat16 or wider, within the bound.
A program may use at most 128 MiB of HBM per device.

```python
import math
import jax
import jax.numpy as jnp
import numpy as np
from jax import lax

D = 2880
HEAD_DIM = 64
HEADS = 32
KV_HEADS = 4
TOK_DEV = 128
QDIM = 2048
KVDIM = 256
SHARDS = 32
GROUPS = 4
GTOK = 4096
BLOCK = 4
DOCS = 16
DOC_MOST = 1024


def shared_keyval(key):
    base_draw = jax.random.normal(jax.random.fold_in(key, 5), (D, 2 * KVDIM), jnp.float32) * D ** (-0.5)
    return jnp.clip(base_draw, -1.0, 1.0)


def draw_keyval_weight(key, part):
    return shared_keyval(key).astype(jnp.bfloat16)


def draw_query_weight(key, part):
    base_draw = jax.random.normal(jax.random.fold_in(key, 7), (D, QDIM), jnp.float32) * D ** (-0.5)
    return jnp.clip(base_draw, -4.0, 4.0).astype(jnp.bfloat16)


def draw_hidden(key, part):
    base_draw = jax.random.normal(jax.random.fold_in(key, 3), (GROUPS, GTOK, D), jnp.float32)
    return jnp.clip(base_draw, -8.0, 8.0).astype(jnp.bfloat16)


def draw_loss_mask(key, part):
    places = jnp.arange(GROUPS * GTOK, dtype=jnp.int32).reshape(GROUPS, GTOK)
    threshold = 200 + 600 * places // (GROUPS * GTOK)
    drawn = jax.random.randint(jax.random.fold_in(key, 9), (GROUPS, GTOK), 0, 1000, dtype=jnp.int32)
    flag_values = (drawn < threshold).astype(jnp.int32)
    return flag_values.at[:, -1].set(1)


def profile(amount, total, most, lean):
    loads = [(1 << 20) // math.isqrt(rank ** lean) + 1 for rank in range(2, amount + 1)]
    rest, holding = total - most - (amount - 1), [1] * (amount - 1)
    while rest > 0:
        movable = [i for i in range(amount - 1) if holding[i] < most]
        whole, remaining = sum([loads[i] for i in movable]), rest
        for i in movable:
            extra = min(most - holding[i], max(1, remaining * loads[i] // whole), rest)
            holding[i] = holding[i] + extra
            rest = rest - extra
    return np.array([most] + holding)


def uneven(own_key, number_of, total, limit, skew):
    if number_of == 2:
        one = jax.random.randint(own_key, (), max(1, total - limit), min(limit, total - 1) + 1)
        return jnp.stack([one, total - one])
    lengths = jnp.asarray(profile(number_of, total, limit, skew), jnp.int32)
    twos = (number_of - 1) // 2
    giver, taker = lengths[1:1 + 2 * twos:2], lengths[2:2 + 2 * twos:2]
    slack = jnp.minimum(giver - 1, limit - taker)
    shifted = jax.random.randint(jax.random.fold_in(own_key, 1), (twos,), 0, 1 << 20) % (slack + 1)
    lengths = lengths.at[1:1 + 2 * twos:2].set(giver - shifted).at[2:2 + 2 * twos:2].set(taker + shifted)
    return lengths[jax.random.permutation(jax.random.fold_in(own_key, 2), number_of)]


def setup_inputs(seed: int = 0) -> dict:
    seeds = jax.random.split(jax.random.key(seed), 9)
    return {
        "hidden": draw_hidden(jax.random.fold_in(seeds[8], 71), 0),
        "norm_gain": jnp.clip(1.0 + 0.1 * jax.random.normal(seeds[1], (D,), jnp.float32), 0.5, 1.5),
        "query_weight": draw_query_weight(jax.random.fold_in(seeds[8], 71), 0),
        "keyval_weight": draw_keyval_weight(jax.random.fold_in(seeds[8], 71), 0),
        "sink_logits": jnp.clip(jax.random.uniform(seeds[4], (HEADS,), jnp.float32, -1.0, 3.0), -1.0, 3.0),
        "document_ids": jax.vmap(lambda own: jnp.searchsorted(jnp.cumsum(uneven(own, DOCS, GTOK, DOC_MOST, 2)), jnp.arange(GTOK), side="right"))(jax.random.split(seeds[5], GROUPS)).reshape((GROUPS, GTOK)).astype(jnp.int32),
        "block_owner": jax.vmap(lambda own: jax.random.permutation(own, SHARDS))(jax.random.split(seeds[6], GROUPS * SHARDS)).reshape((GROUPS, SHARDS, SHARDS)).astype(jnp.int32),
        "loss_mask": draw_loss_mask(jax.random.fold_in(seeds[8], 71), 0),
    }


rope_base = 150000.0
norm_eps = 1e-05
masked_score = -1e+30

def rotate(values, within):
    half_dim = values.shape[-1] // 2
    frequency = jnp.power(rope_base, -jnp.arange(half_dim, dtype=jnp.float32) / half_dim)
    angles = within.astype(jnp.float32)[:, None, None] * frequency[None, None, :]
    cosine = jnp.cos(angles)
    sine_part = jnp.sin(angles)
    first = values[..., :half_dim]
    second = values[..., half_dim:]
    return jnp.concatenate([first * cosine - second * sine_part, second * cosine + first * sine_part], axis=-1)

def doc_within(doc_index):
    length = doc_index.shape[0]
    places = jnp.arange(length, dtype=jnp.int32)
    fresh_doc = jnp.concatenate([jnp.ones((1,), dtype=bool), doc_index[1:] != doc_index[:-1]])
    starts = lax.cummax(jnp.where(fresh_doc, places, 0), axis=0)
    return (places - starts).astype(jnp.int32)

def one_group(rows, doc_index, owner_rows, norm_gain, query_weight, keyval_weight, sink_logits):
    rows_float = rows.astype(jnp.float32)
    inv_rms = lax.rsqrt(lax.optimization_barrier(jnp.mean(rows_float * rows_float, axis=1, keepdims=True)) + norm_eps)
    normed = (rows_float * inv_rms * norm_gain).astype(jnp.bfloat16)
    within = doc_within(doc_index)
    projected = jnp.dot(normed, query_weight, preferred_element_type=jnp.float32).reshape(GTOK, HEADS, HEAD_DIM)
    queries = rotate(projected, within).astype(jnp.bfloat16)
    keyval = jnp.dot(normed, keyval_weight, preferred_element_type=jnp.float32)
    keys_rot = rotate(keyval[:, :KVDIM].reshape(GTOK, KV_HEADS, HEAD_DIM), within).astype(jnp.bfloat16)
    values = keyval[:, KVDIM:].reshape(GTOK, KV_HEADS, HEAD_DIM).astype(jnp.bfloat16)
    group_size = HEADS // KV_HEADS
    keys_float = keys_rot.astype(jnp.float32)
    values_float = values.astype(jnp.float32)
    places = jnp.arange(GTOK, dtype=jnp.int32)
    query_rows = min(512, GTOK)
    score_scale = HEAD_DIM ** (-0.5)

    def query_block(first_row):
        query_part = lax.dynamic_slice_in_dim(queries, first_row, query_rows, 0).astype(jnp.float32)
        query_part = query_part.reshape(query_rows, KV_HEADS, group_size, HEAD_DIM)
        scores = jnp.einsum('qagd,kad->agqk', query_part, keys_float).reshape(HEADS, query_rows, GTOK) * score_scale
        query_place = first_row + jnp.arange(query_rows, dtype=jnp.int32)
        query_doc = lax.dynamic_slice_in_dim(doc_index, first_row, query_rows, 0)
        allowed = (query_doc[:, None] == doc_index[None, :]) & (places[None, :] <= query_place[:, None])
        scores = jnp.where(allowed[None], scores, masked_score)
        row_top = jnp.maximum(sink_logits[:, None], lax.optimization_barrier(jnp.max(scores, axis=-1)))
        exp_scores = jnp.exp(scores - row_top[..., None])
        row_total = jnp.exp(sink_logits[:, None] - row_top) + lax.optimization_barrier(jnp.sum(exp_scores, axis=-1))
        rounded = lax.optimization_barrier(exp_scores.astype(jnp.bfloat16))
        weights = rounded.astype(jnp.float32).reshape(KV_HEADS, group_size, query_rows, GTOK)
        mixed_values = jnp.einsum('agqk,kad->agqd', weights, values_float).reshape(HEADS, query_rows, HEAD_DIM)
        normalized = mixed_values / row_total[..., None]
        normalized = jnp.transpose(normalized, (1, 0, 2)).reshape(query_rows, QDIM).astype(jnp.bfloat16)
        return (normalized, row_top + jnp.log(row_total))
    starts = jnp.arange(0, GTOK, query_rows, dtype=jnp.int32)
    outputs, log_totals = lax.map(query_block, starts)
    attended = outputs.reshape(GTOK, QDIM)
    log_total = jnp.transpose(log_totals, (1, 0, 2)).reshape(HEADS, GTOK)
    inverse = jnp.argsort(owner_rows, axis=1).astype(jnp.int32)
    source_shard = jnp.arange(SHARDS, dtype=jnp.int32)[None, :, None]
    inner_rows = jnp.arange(BLOCK, dtype=jnp.int32)[None, None, :]
    source = source_shard * TOK_DEV + jnp.transpose(inverse)[:, :, None] * BLOCK + inner_rows
    row_lse = jnp.take(log_total, source.reshape(-1).astype(jnp.int32), axis=1)
    return (attended, row_lse)

def reference(hidden, norm_gain, query_weight, keyval_weight, sink_logits, document_ids, block_owner, loss_mask):
    attended_list = []
    lse_list = []
    for group_index in range(GROUPS):
        attended, row_lse = one_group(hidden[group_index], document_ids[group_index], block_owner[group_index], norm_gain, query_weight, keyval_weight, sink_logits)
        attended_list.append(attended)
        lse_list.append(row_lse)
    flag_values = loss_mask.astype(jnp.float32)
    token_total = jnp.sum(flag_values)
    token_weight = flag_values * (float(GROUPS * GTOK) / token_total)
    return (jnp.stack(attended_list), jnp.stack(lse_list), token_weight)
```

```python
import functools
import math

import jax
import jax.numpy as jnp
import numpy as np
from jax import lax
from jax.experimental import pallas as pl
from jax.experimental.pallas import tpu as pltpu
from jax.sharding import PartitionSpec as P

MESH = pl.DeviceIdType.MESH
HEAD_DIM = 64
DOC_MOST = 1024
ROPE_BASE = 150000.0
NORM_EPS = 1e-05
MASKED = -1e30
LOG2E = 1.4426950408889634
LN2 = 0.6931471805599453
F32 = jnp.float32
BF16 = jnp.bfloat16
NT = (((1,), (1,)), ((), ()))
Q_CHUNK = 256


def iota(shape, dim):
    return lax.broadcasted_iota(jnp.int32, shape, dim)


def exact_dot(a, b, dims=(((1,), (0,)), ((), ()))):
    return lax.dot_general(a, b, dims, precision=lax.Precision.HIGHEST, preferred_element_type=F32)


def cos_sin(angle):
    k = jnp.floor(angle * (2.0 / math.pi) + 0.5)
    r = ((angle - k * 1.5703125) - k * 4.837512969970703125e-4) - k * 7.549789954891882e-8
    z = r * r
    s = ((-1.9515295891e-4 * z + 8.3321608736e-3) * z - 1.6666654611e-1) * z * r + r
    c = ((2.443315711809948e-5 * z - 1.388731625493765e-3) * z + 4.166664568298827e-2) * z * z - 0.5 * z + 1.0
    q = k.astype(jnp.int32) & 3
    odd = (q & 1) == 1
    cosine = jnp.where(odd, s, c)
    sine = jnp.where(odd, c, s)
    cosine = jnp.where((q == 1) | (q == 2), -cosine, cosine)
    sine = jnp.where(q >= 2, -sine, sine)
    return cosine, sine


def swap_halves(x, low):
    return jnp.where(low, pltpu.roll(x, 96, 1), pltpu.roll(x, 32, 1))


def kernel(
    shape,
    groups,
    hidden_hbm, gain_hbm, qw_hbm, kvw_hbm, sink_ref, docs_ref, owner_ref, mask_ref, freq_ref,
    att_ref, lse_out_ref, tw_ref,
    hid, gain, kvw, qw, normed, qraw, qz, kbuf, vbuf, bias,
    docs_buf, cnt_send, cnt_buf, m_ref, acc_ref, lse_ref, comb_send, comb,
    load_sem, qw_sem,
    doc_ssem, doc_rsem, kv_ssem, kv_rsem, cnt_ssem, cnt_rsem, lse_ssem, lse_rsem,
):
    rows, width, heads, kv_heads, shards, dps = shape
    back = DOC_MOST // rows
    per_kv = heads // kv_heads
    block_rows = rows // shards
    me = lax.axis_index("cp")
    my_dp = lax.axis_index("dp")
    qdim = heads * HEAD_DIM
    n_chunks = qdim // Q_CHUNK
    pairs = heads // 2

    def ahead(k):
        return lax.rem(me + k, shards)

    loads = [
        pltpu.make_async_copy(hidden_hbm, hid, load_sem.at[0]),
        pltpu.make_async_copy(gain_hbm, gain, load_sem.at[1]),
        pltpu.make_async_copy(kvw_hbm, kvw, load_sem.at[2]),
    ]
    for c in loads:
        c.start()
    q_loads = [
        pltpu.make_async_copy(qw_hbm.at[:, pl.ds(i * Q_CHUNK, Q_CHUNK)], qw.at[i], qw_sem.at[i])
        for i in range(n_chunks)
    ]
    for c in q_loads:
        c.start()

    barrier = pltpu.get_barrier_semaphore()

    def greet(k, carry):
        pl.semaphore_signal(barrier, inc=1, device_id={"cp": ahead(k)}, device_id_type=MESH)
        return carry

    lax.fori_loop(1, shards, greet, 0)
    for k in range(1, dps):
        pl.semaphore_signal(
            barrier, inc=1, device_id={"dp": lax.rem(my_dp + k, dps)}, device_id_type=MESH
        )

    own_docs = docs_ref[...]
    docs_buf[back] = own_docs
    flags = mask_ref[...].astype(F32)
    cnt_row = jnp.broadcast_to(jnp.sum(flags, axis=1, keepdims=True), (1, rows))
    cnt_send[0] = cnt_row
    cnt_buf[0] = cnt_row

    loads[0].wait()
    loads[1].wait()
    x = hid[...].astype(F32)
    inv = lax.rsqrt(jnp.sum(x * x, axis=1, keepdims=True) * (1.0 / width) + NORM_EPS)
    normed[...] = (x * inv * gain[...]).astype(BF16)

    loads[2].wait()
    kv = jnp.dot(normed[...], kvw[...], preferred_element_type=F32)
    kv_width = kv_heads * HEAD_DIM
    for t in range(kv_heads // 2):
        v_t = kv[:, kv_width + t * 128:kv_width + (t + 1) * 128].T.astype(BF16)
        vbuf[back, 2 * t] = v_t[:HEAD_DIM]
        vbuf[back, 2 * t + 1] = v_t[HEAD_DIM:]

    pl.semaphore_wait(barrier, shards - 1 + dps - 1)

    sends = []

    def send(src, dst, ssem, rsem, device):
        c = pltpu.make_async_remote_copy(
            src_ref=src, dst_ref=dst, send_sem=ssem, recv_sem=rsem,
            device_id=device, device_id_type=MESH,
        )
        c.start()
        sends.append(c)
        return c

    doc_copies = {}
    for k in range(1, back + 1):
        doc_copies[k] = send(
            docs_buf.at[back], docs_buf.at[back - k], doc_ssem.at[k - 1], doc_rsem.at[k - 1],
            {"cp": ahead(k)},
        )
    cnt_copies = []
    for k in range(1, dps):
        cnt_copies.append(send(
            cnt_send.at[0], cnt_buf.at[k], cnt_ssem.at[k - 1], cnt_rsem.at[k - 1],
            {"dp": lax.rem(my_dp + k, dps)},
        ))
    v_copies, k_copies = {}, {}
    for k in range(1, back + 1):
        v_copies[k] = send(
            vbuf.at[back], vbuf.at[back - k], kv_ssem.at[0, k - 1], kv_rsem.at[0, k - 1], {"cp": ahead(k)}
        )

    for i in range(n_chunks):
        q_loads[i].wait()
        qraw[:, i * Q_CHUNK:(i + 1) * Q_CHUNK] = jnp.dot(normed[...], qw[i], preferred_element_type=F32)

    for k in range(1, back + 1):
        doc_copies[k].wait_recv()
    square = (rows, 128)
    lane = iota(square, 1)
    sub = iota(square, 0)
    own_row = jnp.broadcast_to(own_docs.astype(F32), square)
    own_col = own_row.T
    count = jnp.zeros(square, F32)
    for b in range(back + 1):
        window_docs = docs_buf[b].astype(F32)
        if b < back:
            window_docs = jnp.where(me >= back - b, window_docs, -1.0)
        count = count + (jnp.broadcast_to(window_docs, square) < own_col).astype(F32)
    start_col = jnp.broadcast_to(jnp.sum(count, axis=1, keepdims=True), square)
    within = (sub + back * rows).astype(F32) - start_col
    cosine, sine = cos_sin(within * freq_ref[...])
    low = (lane % HEAD_DIM) < HEAD_DIM // 2
    sine = jnp.where(low, -sine, sine)

    for t in range(kv_heads // 2):
        u = kv[:, t * 128:(t + 1) * 128]
        kbuf[back, t] = (u * cosine + swap_halves(u, low) * sine).astype(BF16)
    for k in range(1, back + 1):
        k_copies[k] = send(
            kbuf.at[back], kbuf.at[back - k], kv_ssem.at[1, k - 1], kv_rsem.at[1, k - 1], {"cp": ahead(k)}
        )

    scale = HEAD_DIM ** (-0.5)
    q_cos, q_sin = cosine * scale, sine * scale
    left = lane < HEAD_DIM
    for j in range(pairs):
        u = qraw[:, j * 128:(j + 1) * 128]
        y = u * q_cos + swap_halves(u, low) * q_sin
        a = (2 * j) // per_kv
        if a % 2 == 0:
            even = jnp.where(left, y, 0.0)
            odd = jnp.where(left, pltpu.roll(y, 64, 1), 0.0)
        else:
            even = jnp.where(left, 0.0, pltpu.roll(y, 64, 1))
            odd = jnp.where(left, 0.0, y)
        qz[j, :rows] = even.astype(BF16)
        qz[j, rows:] = odd.astype(BF16)

    start_row = start_col.T
    for b in range(back + 1):
        place = (sub + b * rows).astype(F32)
        allowed = place >= start_row
        if b == back:
            allowed = allowed & (sub <= lane)
        bias[b] = jnp.where(allowed, 0.0, MASKED)

    ones_rows = jnp.ones((16, 128), BF16)
    pair_lane = iota((1, 2 * rows), 1) < rows
    acc_rows = HEAD_DIM + 16
    for gi, group in enumerate(groups):
        for b in group:
            if b < back:
                v_copies[back - b].wait_recv()
                k_copies[back - b].wait_recv()
        first, last = gi == 0, gi == len(groups) - 1

        def one_pair(j, carry, group=group, first=first, last=last):
            a = j // (per_kv // 2)
            q2 = qz[j]
            scores = []
            top = None
            for b in group:
                s = lax.dot_general(kbuf[b, a // 2], q2, NT, preferred_element_type=F32)
                bb = bias[b]
                s = s * LOG2E + jnp.concatenate([bb, bb], axis=1)
                scores.append(s)
                part = jnp.max(s.reshape(rows // 8, 8, 2 * rows), axis=0)
                top = part if top is None else jnp.maximum(top, part)
            top = jnp.max(top, axis=0, keepdims=True)
            if first:
                old = jnp.where(pair_lane, sink_ref[2 * j], sink_ref[2 * j + 1]) * LOG2E
            else:
                old = m_ref[j][:1]
            new = jnp.maximum(old, top)
            weights = [jnp.exp2(s - new).astype(BF16) for s in scores]
            vt = jnp.concatenate([jnp.concatenate([vbuf[b, a], ones_rows], axis=0) for b in group], axis=1)
            mixed = jnp.dot(vt, jnp.concatenate(weights, axis=0), preferred_element_type=F32)
            shrink = jnp.exp2(old - new)
            if first:
                acc = mixed + jnp.where(iota((acc_rows, 2 * rows), 0) >= HEAD_DIM, shrink, 0.0)
            else:
                acc = acc_ref[j] * shrink + mixed
            if last:
                total = acc[HEAD_DIM:HEAD_DIM + 1]
                out = acc[:HEAD_DIM] * (1.0 / total)
                out = jnp.concatenate([out[:, :rows], out[:, rows:]], axis=0).T
                att_ref[:, pl.ds(pl.multiple_of(j * 128, 128), 128)] = out.astype(BF16)
                lse = (new + jnp.log2(total)) * LN2
                lse_ref[pl.ds(2 * j, 1), :] = lse[:, :rows]
                lse_ref[pl.ds(2 * j + 1, 1), :] = lse[:, rows:]
            else:
                acc_ref[j] = acc
                m_ref[j] = jnp.broadcast_to(new, (8, 2 * rows))
            return carry

        lax.fori_loop(0, pairs, one_pair, 0)

    for c in cnt_copies:
        c.wait_recv()
    cnt = cnt_buf[0]
    for k in range(1, dps):
        cnt = cnt + cnt_buf[k]

    spread = (iota((shards, rows), 1) // block_rows == iota((shards, rows), 0)).astype(F32)
    owner_row = jnp.broadcast_to(owner_ref[...].astype(F32), (8, shards))
    owner_wide = exact_dot(owner_row, spread)[:1]
    chosen = (jnp.broadcast_to(owner_wide, (shards, rows)) == iota((shards, rows), 0).astype(F32)).astype(F32)
    wide = block_rows * heads
    lse4 = jnp.concatenate([lse_ref[...]] * block_rows, axis=0)
    lse4 = jnp.where(iota((wide, rows), 1) % block_rows == iota((wide, rows), 0) // heads, lse4, 0.0)
    rows_out = exact_dot(chosen, lse4, NT)
    comb_send[:, 0, :] = rows_out
    comb_send[:, 1, :] = jnp.broadcast_to(cnt, (shards, rows))
    comb[me] = comb_send[me]

    def lse_copy(k):
        return pltpu.make_async_remote_copy(
            src_ref=comb_send.at[ahead(k)], dst_ref=comb.at[me],
            send_sem=lse_ssem.at[k], recv_sem=lse_rsem.at[k],
            device_id={"cp": ahead(k)}, device_id_type=MESH,
        )

    def lse_send(k, carry):
        lse_copy(k).start()
        return carry

    def lse_wait(k, carry):
        lse_copy(k).wait_recv()
        return carry

    def lse_done(k, carry):
        lse_copy(k).wait_send()
        return carry

    lax.fori_loop(1, shards, lse_send, 0)
    lax.fori_loop(1, shards, lse_wait, 0)

    got = comb[:, 0, :]
    totals = jnp.sum(comb[:, 1, :], axis=0, keepdims=True)
    back_spread = (iota((rows, shards), 0) // block_rows == iota((rows, shards), 1)).astype(F32)
    wide_got = exact_dot(back_spread, got)
    wide_got = jnp.where(iota((rows, wide), 0) % block_rows == iota((rows, wide), 1) // heads, wide_got, 0.0)
    pick = (iota((heads, wide), 1) % heads == iota((heads, wide), 0)).astype(F32)
    lse_out_ref[...] = exact_dot(pick, wide_got, NT)
    tw_ref[...] = flags * (float(dps * shards * rows) / totals)

    for c in sends:
        c.wait_send()
    lax.fori_loop(1, shards, lse_done, 0)


def solution(mesh):
    dps, shards = mesh.shape["dp"], mesh.shape["cp"]
    half = HEAD_DIM // 2
    freq_np = ROPE_BASE ** (-(np.arange(128) % half).astype(np.float64) / half)

    def body(hidden, norm_gain, query_weight, keyval_weight, sink_logits, document_ids, block_owner, loss_mask):
        rows, width = hidden.shape[1:]
        heads = sink_logits.shape[0]
        kv_heads = keyval_weight.shape[1] // (2 * HEAD_DIM)
        qdim = heads * HEAD_DIM
        back = DOC_MOST // rows
        slots = back + 1
        pairs = heads // 2
        groups = ((back,), tuple(range(back - 1, back // 2 - 1, -1)), tuple(range(back // 2 - 1, -1, -1)))
        shape = (rows, width, heads, kv_heads, shards, dps)
        any_spec = pl.BlockSpec(memory_space=pl.ANY)
        vm = pl.BlockSpec(memory_space=pltpu.VMEM)
        dma = pltpu.SemaphoreType.DMA
        att, lse, tw = pl.pallas_call(
            functools.partial(kernel, shape, groups),
            name="attention_step",
            out_shape=(
                jax.ShapeDtypeStruct((rows, qdim), BF16),
                jax.ShapeDtypeStruct((heads, rows), F32),
                jax.ShapeDtypeStruct((1, rows), F32),
            ),
            in_specs=[any_spec] * 4 + [pl.BlockSpec(memory_space=pltpu.SMEM)] + [vm] * 4,
            out_specs=(vm, vm, vm),
            scratch_shapes=[
                pltpu.VMEM((rows, width), BF16),
                pltpu.VMEM((1, width), F32),
                pltpu.VMEM((width, keyval_weight.shape[1]), BF16),
                pltpu.VMEM((qdim // Q_CHUNK, width, Q_CHUNK), BF16),
                pltpu.VMEM((rows, width), BF16),
                pltpu.VMEM((rows, qdim), F32),
                pltpu.VMEM((pairs, 2 * rows, 128), BF16),
                pltpu.VMEM((slots, kv_heads // 2, rows, 128), BF16),
                pltpu.VMEM((slots, kv_heads, HEAD_DIM, rows), BF16),
                pltpu.VMEM((slots, rows, rows), F32),
                pltpu.VMEM((slots, 1, rows), jnp.int32),
                pltpu.VMEM((1, 1, rows), F32),
                pltpu.VMEM((dps, 1, rows), F32),
                pltpu.VMEM((pairs, 8, 2 * rows), F32),
                pltpu.VMEM((pairs, HEAD_DIM + 16, 2 * rows), F32),
                pltpu.VMEM((heads, rows), F32),
                pltpu.VMEM((shards, 2, rows), F32),
                pltpu.VMEM((shards, 2, rows), F32),
                dma((3,)), dma((qdim // Q_CHUNK,)),
                dma((back,)), dma((back,)),
                dma((2, back)), dma((2, back)),
                dma((dps,)), dma((dps,)),
                dma((shards,)), dma((shards,)),
            ],
            compiler_params=pltpu.CompilerParams(
                collective_id=0, has_side_effects=True, vmem_limit_bytes=56 * 1024 * 1024
            ),
        )(
            hidden[0], norm_gain.reshape(1, width), query_weight, keyval_weight, sink_logits,
            document_ids, block_owner[0], loss_mask,
            jnp.asarray(freq_np.reshape(1, 128), F32),
        )
        return att[None], lse[None], tw

    return jax.shard_map(
        body,
        mesh=mesh,
        in_specs=(
            P("dp", "cp", None), P(), P(), P(), P(), P("dp", "cp"), P("dp", "cp", None), P("dp", "cp"),
        ),
        out_specs=(P("dp", "cp", None), P("dp", None, "cp"), P("dp", "cp")),
        check_vma=False,
    )
```

```python
import functools
import math

import jax
import jax.numpy as jnp
import numpy as np
from jax import lax
from jax.experimental import pallas as pl
from jax.experimental.pallas import tpu as pltpu
from jax.sharding import PartitionSpec as P

MESH = pl.DeviceIdType.MESH
HEAD_DIM = 64
DOC_MOST = 1024
ROPE_BASE = 150000.0
NORM_EPS = 1e-05
MASKED = -1e30
LOG2E = 1.4426950408889634
LN2 = 0.6931471805599453
F32 = jnp.float32
BF16 = jnp.bfloat16
NT = (((1,), (1,)), ((), ()))
Q_CHUNK = 512
HEADS_STEP = 4
DOC_AT = 1


def iota(shape, dim):
    return lax.broadcasted_iota(jnp.int32, shape, dim)


def exact_dot(a, b, dims=(((1,), (0,)), ((), ()))):
    return lax.dot_general(a, b, dims, precision=lax.Precision.HIGHEST, preferred_element_type=F32)


def cos_sin(angle):
    k = jnp.floor(angle * (2.0 / math.pi) + 0.5)
    r = ((angle - k * 1.5703125) - k * 4.837512969970703125e-4) - k * 7.549789954891882e-8
    z = r * r
    s = ((-1.9515295891e-4 * z + 8.3321608736e-3) * z - 1.6666654611e-1) * z * r + r
    c = ((2.443315711809948e-5 * z - 1.388731625493765e-3) * z + 4.166664568298827e-2) * z * z - 0.5 * z + 1.0
    q = k.astype(jnp.int32) & 3
    odd = (q & 1) == 1
    cosine = jnp.where(odd, s, c)
    sine = jnp.where(odd, c, s)
    cosine = jnp.where((q == 1) | (q == 2), -cosine, cosine)
    sine = jnp.where(q >= 2, -sine, sine)
    return cosine, sine


def kernel(
    shape,
    groups,
    hidden_hbm, gain_hbm, qw_hbm, kvw_hbm, sink_hbm, docs_hbm, owner_hbm, mask_hbm, freq_hbm,
    att_hbm, lse_hbm, tw_hbm,
    hid, gain, kvw, qw, normed, qt, qz, kbuf, vbuf, bias,
    docs_buf, cnt_send, cnt_buf, m_ref, acc_ref, lse_ref, comb_send, comb, s_even, s_odd, top_even, top_odd,
    sink_ref, owner_ref, mask_ref, freq_ref, att_ref, lse_out_ref, tw_ref,
    load_sem, qw_sem,
    doc_ssem, doc_rsem, kv_ssem, kv_rsem, cnt_ssem, cnt_rsem, lse_ssem, lse_rsem,
):
    rows, width, heads, kv_heads, shards, dps = shape
    back = DOC_MOST // rows
    per_kv = heads // kv_heads
    block_rows = rows // shards
    me = lax.axis_index("cp")
    my_dp = lax.axis_index("dp")
    qdim = heads * HEAD_DIM
    n_chunks = qdim // Q_CHUNK
    pairs = heads // HEADS_STEP
    half = HEAD_DIM // 2

    def ahead(k):
        return lax.rem(me + k, shards)

    loads = [
        pltpu.make_async_copy(hidden_hbm, hid, load_sem.at[0]),
        pltpu.make_async_copy(gain_hbm, gain, load_sem.at[1]),
        pltpu.make_async_copy(docs_hbm, docs_buf.at[back], load_sem.at[2]),
        pltpu.make_async_copy(mask_hbm, mask_ref, load_sem.at[3]),
        pltpu.make_async_copy(kvw_hbm, kvw, load_sem.at[4]),
        pltpu.make_async_copy(freq_hbm, freq_ref, load_sem.at[5]),
        pltpu.make_async_copy(sink_hbm, sink_ref, load_sem.at[6]),
        pltpu.make_async_copy(owner_hbm, owner_ref, load_sem.at[7]),
    ]
    for c in loads:
        c.start()

    barrier = pltpu.get_barrier_semaphore()

    def greet(k, carry):
        pl.semaphore_signal(barrier, inc=1, device_id={"cp": ahead(k)}, device_id_type=MESH)
        return carry

    lax.fori_loop(1, shards, greet, 0)
    for k in range(1, dps):
        pl.semaphore_signal(
            barrier, inc=1, device_id={"dp": lax.rem(my_dp + k, dps)}, device_id_type=MESH
        )

    loads[0].wait()
    loads[1].wait()
    q_loads = [
        pltpu.make_async_copy(qw_hbm.at[:, pl.ds(i * Q_CHUNK, Q_CHUNK)], qw.at[i], qw_sem.at[i])
        for i in range(n_chunks)
    ]
    for c in q_loads:
        c.start()
    loads[2].wait()
    loads[3].wait()
    own_docs = docs_buf[back]
    flags = mask_ref[...].astype(F32)
    cnt_row = jnp.broadcast_to(jnp.sum(flags, axis=1, keepdims=True), (1, rows))
    cnt_send[0] = cnt_row
    cnt_buf[0] = cnt_row
    x = hid[...].T.astype(F32)
    inv = lax.rsqrt(jnp.sum(x * x, axis=1, keepdims=True) * (1.0 / width) + NORM_EPS)
    normed[...] = (x * inv * gain[...].reshape(1, width)).astype(BF16)

    pl.semaphore_wait(barrier, shards - 1 + dps - 1)

    sends = []

    def send(src, dst, ssem, rsem, device):
        c = pltpu.make_async_remote_copy(
            src_ref=src, dst_ref=dst, send_sem=ssem, recv_sem=rsem,
            device_id=device, device_id_type=MESH,
        )
        c.start()
        sends.append(c)
        return c

    doc_copies = {}
    for k in range(1, back + 1):
        doc_copies[k] = send(
            docs_buf.at[back], docs_buf.at[back - k], doc_ssem.at[k - 1], doc_rsem.at[k - 1],
            {"cp": ahead(k)},
        )
    cnt_copies = []
    for k in range(1, dps):
        cnt_copies.append(send(
            cnt_send.at[0], cnt_buf.at[k], cnt_ssem.at[k - 1], cnt_rsem.at[k - 1],
            {"dp": lax.rem(my_dp + k, dps)},
        ))

    core = lax.rem(me, 2)
    chips = back // 2
    z = lax.rem(me // 2, chips)
    corner = me - 2 * z
    bufs = (vbuf, kbuf)

    def slot_copy(t, src, dst, sem, device):
        buf = bufs[t]
        return pltpu.make_async_remote_copy(
            src_ref=buf.at[src], dst_ref=buf.at[dst], send_sem=kv_ssem.at[t, sem],
            recv_sem=kv_rsem.at[t, dst], device_id={"cp": device}, device_id_type=MESH,
        )

    def row_copy(t, k, src):
        return slot_copy(t, src, back - 2 * k, k, corner + 2 * lax.rem(z + k, chips))

    def next_row_copy(t):
        return slot_copy(t, back, 0, 0, ahead(back))

    def partner_copy(t, src, dst):
        return slot_copy(t, src, dst, chips + src // 2 if src != back else chips, me + 1 - 2 * core)

    def send_own(t):
        @pl.when(core == 0)
        def _():
            partner_copy(t, back, back - 1).start()

        next_row_copy(t).start()
        for k in range(1, chips):
            @pl.when(z + k < chips)
            def _(k=k):
                row_copy(t, k, back).start()

    def arrived(t, slot):
        slot_copy(t, slot, slot, 0, me).wait_recv()

    def serve(t, slot):
        arrived(t, slot)
        if slot == 0:
            for k in range(1, chips):
                @pl.when(z + k >= chips)
                def _(k=k):
                    row_copy(t, k, 0).start()

            @pl.when(core == 1)
            def _():
                partner_copy(t, 0, 1).start()
        else:
            partner_copy(t, slot, slot - 1 + 2 * core).start()

    loads[4].wait()
    kv = jnp.dot(normed[...], kvw[...], preferred_element_type=F32)
    kv_width = kv_heads * HEAD_DIM
    raw_kt = []
    for t in range(kv_heads // 2):
        v_t = kv[:, kv_width + t * 128:kv_width + (t + 1) * 128].T.astype(BF16)
        vbuf[back, 2 * t] = v_t[:HEAD_DIM]
        vbuf[back, 2 * t + 1] = v_t[HEAD_DIM:]
        raw_kt.append(kv[:, t * 128:(t + 1) * 128].T)

    def q_part(i):
        q_loads[i].wait()
        part = jnp.dot(normed[...], qw[i], preferred_element_type=F32)
        for t in range(Q_CHUNK // 128):
            at = i * Q_CHUNK + t * 128
            qt[at:at + 128] = part[:, t * 128:(t + 1) * 128].T

    send_own(0)

    for i in range(DOC_AT):
        q_part(i)

    for k in range(1, back + 1):
        doc_copies[k].wait_recv()
    for i in range(5, 8):
        loads[i].wait()
    square = (rows, 128)
    lane = iota(square, 1)
    sub = iota(square, 0)
    own_row = jnp.broadcast_to(own_docs.astype(F32), square)
    own_col = own_row.T
    count = jnp.zeros(square, F32)
    for b in range(back + 1):
        window_docs = docs_buf[b].astype(F32)
        if b < back:
            window_docs = jnp.where(me >= back - b, window_docs, -1.0)
        count = count + (jnp.broadcast_to(window_docs, square) < own_col).astype(F32)
    start_row = jnp.broadcast_to(jnp.sum(count, axis=1, keepdims=True), square).T
    within = (lane[:half] + back * rows).astype(F32) - start_row[:half]
    cosine, sine = cos_sin(within * freq_ref[...])

    def rope(u):
        a, b = u[:half], u[half:]
        return jnp.concatenate([a * cosine - b * sine, b * cosine + a * sine], axis=0)

    for t in range(kv_heads // 2):
        u = raw_kt[t]
        u = jnp.concatenate([rope(u[:HEAD_DIM]), rope(u[HEAD_DIM:])], axis=0)
        kbuf[back, t] = u.T.astype(BF16)
    send_own(1)

    serve(0, 0)
    for i in range(DOC_AT, 3):
        q_part(i)
    serve(1, 0)
    for i in range(3, n_chunks):
        q_part(i)

    scale = HEAD_DIM ** (-0.5)
    zeros = jnp.zeros((HEAD_DIM, rows), BF16)
    for h in range(heads):
        y = (rope(qt[h * HEAD_DIM:(h + 1) * HEAD_DIM]) * scale).astype(BF16)
        at = (h // per_kv) % 2
        lanes = slice((h % HEADS_STEP) * rows, (h % HEADS_STEP + 1) * rows)
        qz[h // HEADS_STEP, at * HEAD_DIM:(at + 1) * HEAD_DIM, lanes] = y
        qz[h // HEADS_STEP, (1 - at) * HEAD_DIM:(2 - at) * HEAD_DIM, lanes] = zeros

    for b in range(back + 1):
        place = (sub + b * rows).astype(F32)
        allowed = place >= start_row
        if b == back:
            allowed = allowed & (sub <= lane)
        bias[b] = jnp.where(allowed, 0.0, MASKED)

    serve(0, 6)
    serve(1, 6)
    serve(0, 4)
    serve(1, 4)
    serve(0, 2)
    serve(1, 2)
    arrived(0, 7)
    arrived(1, 7)
    arrived(0, 5)
    arrived(1, 5)
    arrived(0, 3)
    arrived(1, 3)
    arrived(0, 1)
    arrived(1, 1)
    two = HEADS_STEP * rows
    head_lane = iota((1, two), 1) // rows
    acc_rows = HEAD_DIM + 16
    for gi, (b0, b1) in enumerate(groups):
        first, last = gi == 0, gi == len(groups) - 1
        nb = b1 - b0
        ones_rows = jnp.ones((16, nb * rows), BF16)

        def score(j, s_ref, t_ref, b0=b0, b1=b1, nb=nb):
            a = j // (per_kv // HEADS_STEP)
            kb = jnp.concatenate([kbuf[b, a // 2] for b in range(b0, b1)], axis=0)
            s = jnp.dot(kb, qz[j], preferred_element_type=F32)
            top = None
            for b in range(nb):
                bb = bias[b0 + b]
                sb = s[b * rows:(b + 1) * rows] * LOG2E + jnp.concatenate([bb] * HEADS_STEP, axis=1)
                s_ref[b * rows:(b + 1) * rows] = sb
                part = jnp.max(sb.reshape(rows // 8, 8, two), axis=0)
                top = part if top is None else jnp.maximum(top, part)
            t_ref[...] = top

        def mix(j, s_ref, t_ref, b0=b0, b1=b1, nb=nb, first=first, last=last, ones_rows=ones_rows):
            a = j // (per_kv // HEADS_STEP)
            top = jnp.max(t_ref[...], axis=0, keepdims=True)
            if first:
                old = jnp.zeros((1, two), F32)
                for i in range(HEADS_STEP):
                    old = jnp.where(head_lane == i, sink_ref[HEADS_STEP * j + i] * LOG2E, old)
            else:
                old = m_ref[j][:1]
            new = jnp.maximum(old, top)
            weights = jnp.exp2(s_ref[:nb * rows] - new).astype(BF16)
            vt = jnp.concatenate([vbuf[b, a] for b in range(b0, b1)], axis=1)
            vt = jnp.concatenate([vt, ones_rows], axis=0)
            mixed = jnp.dot(vt, weights, preferred_element_type=F32)
            shrink = jnp.exp2(old - new)
            if first:
                acc = mixed + jnp.where(iota((acc_rows, two), 0) >= HEAD_DIM, shrink, 0.0)
            else:
                acc = acc_ref[j] * shrink + mixed
            if last:
                total = acc[HEAD_DIM:HEAD_DIM + 1]
                out = acc[:HEAD_DIM] * (1.0 / total)
                lse = (new + jnp.log2(total)) * LN2
                for i in range(0, HEADS_STEP, 2):
                    both = jnp.concatenate([out[:, i * rows:(i + 1) * rows], out[:, (i + 1) * rows:(i + 2) * rows]], axis=0).T
                    at = pl.multiple_of(j * (HEADS_STEP * HEAD_DIM) + i * HEAD_DIM, 128)
                    att_ref[:, pl.ds(at, 128)] = both.astype(BF16)
                for i in range(HEADS_STEP):
                    lse_ref[pl.ds(HEADS_STEP * j + i, 1), :] = lse[:, i * rows:(i + 1) * rows]
            else:
                acc_ref[j] = acc
                m_ref[j] = jnp.broadcast_to(new, (8, two))

        def two_pairs(i, carry, score=score, mix=mix):
            j = 2 * i
            score(j + 1, s_odd, top_odd)
            mix(j, s_even, top_even)
            score(lax.rem(j + 2, pairs), s_even, top_even)
            mix(j + 1, s_odd, top_odd)
            return carry

        with jax.named_scope("loop%d" % gi):
            score(0, s_even, top_even)
            lax.fori_loop(0, pairs // 2, two_pairs, 0)

    att_copy = pltpu.make_async_copy(att_ref, att_hbm, load_sem.at[0])
    att_copy.start()
    for c in cnt_copies:
        c.wait_recv()
    cnt = cnt_buf[0]
    for k in range(1, dps):
        cnt = cnt + cnt_buf[k]

    spread = (iota((shards, rows), 1) // block_rows == iota((shards, rows), 0)).astype(F32)
    owner_row = jnp.broadcast_to(owner_ref[...].astype(F32), (8, shards))
    owner_wide = exact_dot(owner_row, spread)[:1]
    chosen = (jnp.broadcast_to(owner_wide, (shards, rows)) == iota((shards, rows), 0).astype(F32)).astype(F32)
    wide = block_rows * heads
    lse4 = jnp.concatenate([lse_ref[...]] * block_rows, axis=0)
    lse4 = jnp.where(iota((wide, rows), 1) % block_rows == iota((wide, rows), 0) // heads, lse4, 0.0)
    rows_out = exact_dot(chosen, lse4, NT)
    comb_send[:, 0, :] = rows_out
    comb_send[:, 1, :] = jnp.broadcast_to(cnt, (shards, rows))
    comb[me] = comb_send[me]

    def lse_copy(k):
        return pltpu.make_async_remote_copy(
            src_ref=comb_send.at[ahead(k)], dst_ref=comb.at[me],
            send_sem=lse_ssem.at[k], recv_sem=lse_rsem.at[k],
            device_id={"cp": ahead(k)}, device_id_type=MESH,
        )

    def lse_send(k, carry):
        lse_copy(k).start()
        return carry

    def lse_wait(k, carry):
        lse_copy(k).wait_recv()
        return carry

    def lse_done(k, carry):
        lse_copy(k).wait_send()
        return carry

    lax.fori_loop(1, shards, lse_send, 0)
    lax.fori_loop(1, shards, lse_wait, 0)

    got = comb[:, 0, :]
    totals = jnp.sum(comb[:, 1, :], axis=0, keepdims=True)
    back_spread = (iota((rows, shards), 0) // block_rows == iota((rows, shards), 1)).astype(F32)
    wide_got = exact_dot(back_spread, got)
    wide_got = jnp.where(iota((rows, wide), 0) % block_rows == iota((rows, wide), 1) // heads, wide_got, 0.0)
    pick = (iota((heads, wide), 1) % heads == iota((heads, wide), 0)).astype(F32)
    lse_out_ref[...] = exact_dot(pick, wide_got, NT)
    lse_move = pltpu.make_async_copy(lse_out_ref, lse_hbm, load_sem.at[1])
    lse_move.start()
    tw_ref[...] = flags * (float(dps * shards * rows) / totals)
    tw_move = pltpu.make_async_copy(tw_ref, tw_hbm, load_sem.at[2])
    tw_move.start()

    att_copy.wait()
    lse_move.wait()
    tw_move.wait()
    for c in sends:
        c.wait_send()
    for t in range(2):
        for sem in range(2 * chips):
            slot_copy(t, back, 0, sem, me).wait_send()
    lax.fori_loop(1, shards, lse_done, 0)


def store(att_in, lse_in, tw_in, att_out, lse_out, tw_out, att, lse, tw, in_sem, out_sem):
    parts = 4
    step = att.shape[0] // parts
    moves = [(att_in.at[pl.ds(i * step, step)], att.at[pl.ds(i * step, step)], att_out.at[pl.ds(i * step, step)]) for i in range(parts)]
    moves += [(lse_in, lse, lse_out), (tw_in, tw, tw_out)]
    ins = [pltpu.make_async_copy(a, b, in_sem.at[i]) for i, (a, b, c) in enumerate(moves)]
    outs = [pltpu.make_async_copy(b, c, out_sem.at[i]) for i, (a, b, c) in enumerate(moves)]
    for c in ins:
        c.start()
    for i, c in enumerate(outs):
        ins[i].wait()
        c.start()
    for c in outs:
        c.wait()


def solution(mesh):
    dps, shards = mesh.shape["dp"], mesh.shape["cp"]
    half = HEAD_DIM // 2
    freq_np = np.broadcast_to(ROPE_BASE ** (-np.arange(half).astype(np.float64) / half)[:, None], (half, 128))

    def body(hidden, norm_gain, query_weight, keyval_weight, sink_logits, document_ids, block_owner, loss_mask):
        rows, width = hidden.shape[1:]
        heads = sink_logits.shape[0]
        kv_heads = keyval_weight.shape[1] // (2 * HEAD_DIM)
        qdim = heads * HEAD_DIM
        back = DOC_MOST // rows
        slots = back + 1
        pairs = heads // HEADS_STEP
        groups = ((back - 2, back + 1), (back - 5, back - 2), (0, back - 5))
        widest = max(b1 - b0 for b0, b1 in groups) * rows
        shape = (rows, width, heads, kv_heads, shards, dps)
        hbm = pl.BlockSpec(memory_space=pltpu.HBM)
        dma = pltpu.SemaphoreType.DMA
        att, lse, tw = pl.pallas_call(
            functools.partial(kernel, shape, groups),
            name="attention_step",
            out_shape=(
                jax.ShapeDtypeStruct((rows, qdim), BF16),
                jax.ShapeDtypeStruct((heads, rows), F32),
                jax.ShapeDtypeStruct((1, rows), F32),
            ),
            in_specs=[hbm] * 9,
            out_specs=(hbm, hbm, hbm),
            scratch_shapes=[
                pltpu.VMEM((width, rows), BF16),
                pltpu.VMEM((width,), F32),
                pltpu.VMEM((width, keyval_weight.shape[1]), BF16),
                pltpu.VMEM((qdim // Q_CHUNK, width, Q_CHUNK), BF16),
                pltpu.VMEM((rows, width), BF16),
                pltpu.VMEM((qdim, rows), F32),
                pltpu.VMEM((pairs, 128, HEADS_STEP * rows), BF16),
                pltpu.VMEM((slots, kv_heads // 2, rows, 128), BF16),
                pltpu.VMEM((slots, kv_heads, HEAD_DIM, rows), BF16),
                pltpu.VMEM((slots, rows, rows), F32),
                pltpu.VMEM((slots, 1, rows), jnp.int32),
                pltpu.VMEM((1, 1, rows), F32),
                pltpu.VMEM((dps, 1, rows), F32),
                pltpu.VMEM((pairs, 8, HEADS_STEP * rows), F32),
                pltpu.VMEM((pairs, HEAD_DIM + 16, HEADS_STEP * rows), F32),
                pltpu.VMEM((heads, rows), F32),
                pltpu.VMEM((shards, 2, rows), F32),
                pltpu.VMEM((shards, 2, rows), F32),
                pltpu.VMEM((widest, HEADS_STEP * rows), F32),
                pltpu.VMEM((widest, HEADS_STEP * rows), F32),
                pltpu.VMEM((8, HEADS_STEP * rows), F32),
                pltpu.VMEM((8, HEADS_STEP * rows), F32),
                pltpu.SMEM((heads,), F32),
                pltpu.VMEM((1, shards), jnp.int32),
                pltpu.VMEM((1, rows), jnp.int32),
                pltpu.VMEM((half, 128), F32),
                pltpu.VMEM((rows, qdim), BF16),
                pltpu.VMEM((heads, rows), F32),
                pltpu.VMEM((1, rows), F32),
                dma((8,)), dma((qdim // Q_CHUNK,)),
                dma((back,)), dma((back,)),
                dma((2, back)), dma((2, back)),
                dma((dps,)), dma((dps,)),
                dma((shards,)), dma((shards,)),
            ],
            compiler_params=pltpu.CompilerParams(
                collective_id=0, has_side_effects=True, vmem_limit_bytes=58 * 1024 * 1024
            ),
        )(
            hidden[0].T, norm_gain, query_weight, keyval_weight, sink_logits,
            document_ids, block_owner[0], loss_mask,
            jnp.asarray(freq_np, F32),
        )
        results = (att, lse, tw)
        att, lse, tw = pl.pallas_call(
            store,
            name="store_results",
            out_shape=tuple(jax.ShapeDtypeStruct(r.shape, r.dtype) for r in results),
            in_specs=[hbm] * 3,
            out_specs=(hbm,) * 3,
            scratch_shapes=[pltpu.VMEM(r.shape, r.dtype) for r in results] + [dma((6,)), dma((6,))],
            compiler_params=pltpu.CompilerParams(vmem_limit_bytes=58 * 1024 * 1024),
        )(*results)
        return att[None], lse[None], tw

    return jax.shard_map(
        body,
        mesh=mesh,
        in_specs=(
            P("dp", "cp", None), P(), P(), P(), P(), P("dp", "cp"), P("dp", "cp", None), P("dp", "cp"),
        ),
        out_specs=(P("dp", "cp", None), P("dp", None, "cp"), P("dp", "cp")),
        check_vma=False,
    )
```

```python
import functools
import math

import jax
import jax.numpy as jnp
import numpy as np
from jax import lax
from jax.experimental import pallas as pl
from jax.experimental.pallas import tpu as pltpu
from jax.sharding import PartitionSpec as P

MESH = pl.DeviceIdType.MESH
HEAD_DIM = 64
DOC_MOST = 1024
ROPE_BASE = 150000.0
NORM_EPS = 1e-05
MASKED = -1e30
LOG2E = 1.4426950408889634
LN2 = 0.6931471805599453
F32 = jnp.float32
BF16 = jnp.bfloat16
NT = (((1,), (1,)), ((), ()))
Q_CHUNK = 512
HEADS_STEP = 4
DOC_AT = 2


def iota(shape, dim):
    return lax.broadcasted_iota(jnp.int32, shape, dim)


def exact_dot(a, b, dims=(((1,), (0,)), ((), ()))):
    return lax.dot_general(a, b, dims, precision=lax.Precision.HIGHEST, preferred_element_type=F32)


def cos_sin(angle):
    k = jnp.floor(angle * (2.0 / math.pi) + 0.5)
    r = ((angle - k * 1.5703125) - k * 4.837512969970703125e-4) - k * 7.549789954891882e-8
    z = r * r
    s = ((-1.9515295891e-4 * z + 8.3321608736e-3) * z - 1.6666654611e-1) * z * r + r
    c = ((2.443315711809948e-5 * z - 1.388731625493765e-3) * z + 4.166664568298827e-2) * z * z - 0.5 * z + 1.0
    q = k.astype(jnp.int32) & 3
    odd = (q & 1) == 1
    cosine = jnp.where(odd, s, c)
    sine = jnp.where(odd, c, s)
    cosine = jnp.where((q == 1) | (q == 2), -cosine, cosine)
    sine = jnp.where(q >= 2, -sine, sine)
    return cosine, sine


def kernel(
    shape,
    hidden_hbm, gain_hbm, qw_hbm, kvw_hbm, sink_hbm, docs_hbm, owner_hbm, mask_hbm, freq_hbm,
    att_hbm, lse_hbm, tw_hbm,
    hid, gain, kvw, qw, normed, qt, qz, kbuf, vbuf, bias,
    docs_buf, cnt_send, cnt_buf, m_ref, acc_ref, lse_ref, comb_send, comb, s_even, s_odd, top_even, top_odd,
    chosen3, sink_ref, owner_ref, mask_ref, freq_ref, att_ref, lse_out_ref, tw_ref,
    load_sem, qw_sem,
    doc_sem, kv_ssem, kv_rsem, cnt_ssem, cnt_rsem, lse_sem,
):
    rows, width, heads, kv_heads, shards, dps = shape
    back = DOC_MOST // rows
    per_kv = heads // kv_heads
    block_rows = rows // shards
    me = lax.axis_index("cp")
    my_dp = lax.axis_index("dp")
    qdim = heads * HEAD_DIM
    n_chunks = qdim // Q_CHUNK
    pairs = heads // HEADS_STEP
    half = HEAD_DIM // 2

    def ahead(k):
        return lax.rem(me + k, shards)

    loads = [
        pltpu.make_async_copy(hidden_hbm, hid, load_sem.at[0]),
        pltpu.make_async_copy(gain_hbm, gain, load_sem.at[1]),
        pltpu.make_async_copy(docs_hbm, docs_buf.at[back], load_sem.at[2]),
        pltpu.make_async_copy(mask_hbm, mask_ref, load_sem.at[3]),
        pltpu.make_async_copy(kvw_hbm, kvw, load_sem.at[4]),
        pltpu.make_async_copy(freq_hbm, freq_ref, load_sem.at[5]),
        pltpu.make_async_copy(sink_hbm, sink_ref, load_sem.at[6]),
        pltpu.make_async_copy(owner_hbm, owner_ref, load_sem.at[7]),
    ]
    for c in loads:
        c.start()

    barrier = pltpu.get_barrier_semaphore()

    for k in range(1, back + 1):
        for at in (k, shards - k):
            pl.semaphore_signal(barrier, inc=1, device_id={"cp": ahead(at)}, device_id_type=MESH)
    for k in range(1, dps):
        pl.semaphore_signal(
            barrier, inc=1, device_id={"dp": lax.rem(my_dp + k, dps)}, device_id_type=MESH
        )

    loads[0].wait()
    loads[1].wait()
    q_loads = [
        pltpu.make_async_copy(qw_hbm.at[:, pl.ds(i * Q_CHUNK, Q_CHUNK)], qw.at[i], qw_sem.at[i])
        for i in range(n_chunks)
    ]
    for c in q_loads:
        c.start()
    loads[2].wait()
    loads[3].wait()
    own_docs = docs_buf[back]
    flags = mask_ref[...].astype(F32)
    cnt_row = jnp.broadcast_to(jnp.sum(flags, axis=1, keepdims=True), (1, rows))
    cnt_send[0] = cnt_row
    cnt_buf[0] = cnt_row
    x = hid[...].T.astype(F32)
    inv = lax.rsqrt(jnp.sum(x * x, axis=1, keepdims=True) * (1.0 / width) + NORM_EPS)
    normed[...] = (x * inv * gain[...].reshape(1, width)).astype(BF16)

    pl.semaphore_wait(barrier, 2 * back + dps - 1)

    sends = []

    def send(src, dst, ssem, rsem, device, keep=True):
        c = pltpu.make_async_remote_copy(
            src_ref=src, dst_ref=dst, send_sem=ssem, recv_sem=rsem,
            device_id=device, device_id_type=MESH,
        )
        c.start()
        if keep:
            sends.append(c)
        return c

    for k in range(1, back + 1):
        send(docs_buf.at[back], docs_buf.at[back - k], doc_sem.at[0], doc_sem.at[1], {"cp": ahead(k)}, False)
    cnt_copies = []
    for k in range(1, dps):
        cnt_copies.append(send(
            cnt_send.at[0], cnt_buf.at[k], cnt_ssem.at[k - 1], cnt_rsem.at[k - 1],
            {"dp": lax.rem(my_dp + k, dps)},
        ))

    core = lax.rem(me, 2)
    chips = back // 2
    z = lax.rem(me // 2, chips)
    corner = me - 2 * z
    bufs = (vbuf, kbuf)

    def slot_copy(t, src, dst, sem, device):
        buf = bufs[t]
        return pltpu.make_async_remote_copy(
            src_ref=buf.at[src], dst_ref=buf.at[dst], send_sem=kv_ssem.at[t, sem],
            recv_sem=kv_rsem.at[t, dst], device_id={"cp": device}, device_id_type=MESH,
        )

    def row_copy(t, k, src):
        return slot_copy(t, src, back - 2 * k, k, corner + 2 * lax.rem(z + k, chips))

    def next_row_copy(t):
        return slot_copy(t, back, 0, 0, ahead(back))

    def partner_copy(t, src, dst):
        return slot_copy(t, src, dst, chips + src // 2 if src != back else chips, me + 1 - 2 * core)

    def send_own(t):
        @pl.when(core == 0)
        def _():
            partner_copy(t, back, back - 1).start()

        next_row_copy(t).start()
        for k in range(1, chips):
            @pl.when(z + k < chips)
            def _(k=k):
                row_copy(t, k, back).start()

    def arrived(t, slot):
        slot_copy(t, slot, slot, 0, me).wait_recv()

    def serve(t, slot):
        arrived(t, slot)
        if slot == 0:
            for k in range(1, chips):
                @pl.when(z + k >= chips)
                def _(k=k):
                    row_copy(t, k, 0).start()

            @pl.when(core == 1)
            def _():
                partner_copy(t, 0, 1).start()
        else:
            partner_copy(t, slot, slot - 1 + 2 * core).start()

    loads[4].wait()
    kv = jnp.dot(normed[...], kvw[...], preferred_element_type=F32)
    kv_width = kv_heads * HEAD_DIM
    raw_kt = []
    for t in range(kv_heads // 2):
        v_t = kv[:, kv_width + t * 128:kv_width + (t + 1) * 128].T.astype(BF16)
        vbuf[back, 2 * t] = v_t[:HEAD_DIM]
        vbuf[back, 2 * t + 1] = v_t[HEAD_DIM:]
        raw_kt.append(kv[:, t * 128:(t + 1) * 128].T)

    def q_part(i):
        q_loads[i].wait()
        part = jnp.dot(normed[...], qw[i], preferred_element_type=F32)
        for t in range(Q_CHUNK // 128):
            at = i * Q_CHUNK + t * 128
            qt[at:at + 128] = part[:, t * 128:(t + 1) * 128].T

    send_own(0)

    def docs_all():
        part = docs_buf.at[pl.ds(0, back)]
        return pltpu.make_async_remote_copy(
            src_ref=part, dst_ref=part, send_sem=doc_sem.at[0], recv_sem=doc_sem.at[1],
            device_id={"cp": me}, device_id_type=MESH,
        )

    for i in range(DOC_AT):
        q_part(i)

    for i in range(5, 8):
        loads[i].wait()
    spread = (iota((shards, rows), 1) // block_rows == iota((shards, rows), 0)).astype(F32)
    owner_row = jnp.broadcast_to(owner_ref[...].astype(F32), (8, shards))
    owner_wide = exact_dot(owner_row, spread)[:1]
    chosen = jnp.broadcast_to(owner_wide, (shards, rows)) == iota((shards, rows), 0).astype(F32)
    chosen = chosen.astype(F32).astype(BF16)
    chosen3[...] = jnp.concatenate([chosen] * 3, axis=1)

    docs_all().wait_recv()
    square = (rows, 128)
    lane = iota(square, 1)
    sub = iota(square, 0)
    own_row = jnp.broadcast_to(own_docs.astype(F32), square)
    own_col = own_row.T
    count = jnp.zeros(square, F32)
    for b in range(back + 1):
        window_docs = docs_buf[b].astype(F32)
        if b < back:
            window_docs = jnp.where(me >= back - b, window_docs, -1.0)
        count = count + (jnp.broadcast_to(window_docs, square) < own_col).astype(F32)
    start_row = jnp.broadcast_to(jnp.sum(count, axis=1, keepdims=True), square).T
    within = (lane[:half] + back * rows).astype(F32) - start_row[:half]
    cosine, sine = cos_sin(within * freq_ref[...])

    def rope(u):
        a, b = u[:half], u[half:]
        return jnp.concatenate([a * cosine - b * sine, b * cosine + a * sine], axis=0)

    for t in range(kv_heads // 2):
        u = raw_kt[t]
        u = jnp.concatenate([rope(u[:HEAD_DIM]), rope(u[HEAD_DIM:])], axis=0)
        kbuf[back, t] = u.T.astype(BF16)
    send_own(1)

    for i in range(DOC_AT, n_chunks):
        q_part(i)

    serve(0, 0)
    scale = HEAD_DIM ** (-0.5)
    zeros = jnp.zeros((HEAD_DIM, rows), BF16)
    for h in range(heads):
        y = (rope(qt[h * HEAD_DIM:(h + 1) * HEAD_DIM]) * scale).astype(BF16)
        at = (h // per_kv) % 2
        lanes = slice((h % HEADS_STEP) * rows, (h % HEADS_STEP + 1) * rows)
        qz[h // HEADS_STEP, at * HEAD_DIM:(at + 1) * HEAD_DIM, lanes] = y
        qz[h // HEADS_STEP, (1 - at) * HEAD_DIM:(2 - at) * HEAD_DIM, lanes] = zeros

    for b in range(back + 1):
        place = (sub + b * rows).astype(F32)
        allowed = place >= start_row
        if b == back:
            allowed = allowed & (sub <= lane)
        bias[b] = jnp.where(allowed, 0.0, MASKED)

    serve(1, 0)
    extra = 1 + 6 * core
    odds = tuple(b + 1 - 2 * core for b in (6, 4, 2))

    def before_0():
        arrived(0, extra)
        arrived(1, extra)

    def before_1():
        for slot in (6, 4, 2):
            serve(0, slot)
            serve(1, slot)

    def before_2():
        for slot in odds:
            arrived(0, slot)
            arrived(1, slot)

    groups = (
        (before_0, (back, 0, extra)),
        (before_1, (6, 4, 2)),
        (before_2, odds),
    )
    two = HEADS_STEP * rows
    head_lane = iota((1, two), 1) // rows
    acc_rows = HEAD_DIM + 16
    for gi, (before, slots) in enumerate(groups):
        with jax.named_scope("before%d" % gi):
            before()
        first, last = gi == 0, gi == len(groups) - 1
        nb = len(slots)
        ones_rows = jnp.ones((16, nb * rows), BF16)

        def score(j, s_ref, t_ref, slots=slots, nb=nb):
            a = j // (per_kv // HEADS_STEP)
            kb = jnp.concatenate([kbuf[b, a // 2] for b in slots], axis=0)
            s = jnp.dot(kb, qz[j], preferred_element_type=F32)
            top = None
            for b in range(nb):
                bb = bias[slots[b]]
                sb = s[b * rows:(b + 1) * rows] * LOG2E + jnp.concatenate([bb] * HEADS_STEP, axis=1)
                s_ref[b * rows:(b + 1) * rows] = sb
                part = jnp.max(sb.reshape(rows // 8, 8, two), axis=0)
                top = part if top is None else jnp.maximum(top, part)
            t_ref[...] = top

        def mix(j, s_ref, t_ref, slots=slots, nb=nb, first=first, last=last, ones_rows=ones_rows):
            a = j // (per_kv // HEADS_STEP)
            top = jnp.max(t_ref[...], axis=0, keepdims=True)
            if first:
                old = jnp.zeros((1, two), F32)
                for i in range(HEADS_STEP):
                    old = jnp.where(head_lane == i, sink_ref[HEADS_STEP * j + i] * LOG2E, old)
            else:
                old = m_ref[j][:1]
            new = jnp.maximum(old, top)
            mixed = None
            for b in range(0, nb, 2):
                part = slots[b:b + 2]
                n = len(part) * rows
                weights = jnp.exp2(s_ref[b * rows:b * rows + n] - new).astype(BF16)
                vt = jnp.concatenate([vbuf[i, a] for i in part], axis=1)
                vt = jnp.concatenate([vt, ones_rows[:, :n]], axis=0)
                more = jnp.dot(vt, weights, preferred_element_type=F32)
                mixed = more if mixed is None else mixed + more
            shrink = jnp.exp2(old - new)
            if first:
                acc = mixed + jnp.where(iota((acc_rows, two), 0) >= HEAD_DIM, shrink, 0.0)
            else:
                acc = acc_ref[j] * shrink + mixed
            if last:
                total = acc[HEAD_DIM:HEAD_DIM + 1]
                acc_ref[j] = acc
                lse = (new + jnp.log2(total)) * LN2
                for i in range(HEADS_STEP):
                    lse_ref[pl.ds(HEADS_STEP * j + i, 1), :] = lse[:, i * rows:(i + 1) * rows]
            else:
                acc_ref[j] = acc
                m_ref[j] = jnp.broadcast_to(new, (8, two))

        def two_pairs(i, carry, score=score, mix=mix):
            j = 2 * i
            score(j + 1, s_odd, top_odd)
            mix(j, s_even, top_even)
            score(lax.rem(j + 2, pairs), s_even, top_even)
            mix(j + 1, s_odd, top_odd)
            return carry

        with jax.named_scope("loop%d" % gi):
            score(0, s_even, top_even)
            for j in range(0, pairs, 2):
                score(j + 1, s_odd, top_odd)
                mix(j, s_even, top_even)
                if j + 2 < pairs:
                    score(j + 2, s_even, top_even)
                mix(j + 1, s_odd, top_odd)

    for c in cnt_copies:
        c.wait_recv()
    cnt = cnt_buf[0]
    for k in range(1, dps):
        cnt = cnt + cnt_buf[k]

    def pieces(v):
        hi = v.astype(BF16)
        rest = v - hi.astype(F32)
        mid = rest.astype(BF16)
        return [hi, mid, (rest - mid.astype(F32)).astype(BF16)]

    wide = block_rows * heads
    lse4 = jnp.concatenate([lse_ref[...]] * block_rows, axis=0)
    lse4 = jnp.where(iota((wide, rows), 1) % block_rows == iota((wide, rows), 0) // heads, lse4, 0.0)
    lse4 = jnp.concatenate(pieces(lse4), axis=1)
    comb_send[:, 0, :] = lax.dot_general(chosen3[...], lse4, NT, preferred_element_type=F32)
    comb_send[:, 1, :] = jnp.broadcast_to(cnt, (shards, rows))
    comb[me] = comb_send[me]

    def lse_send(k, carry):
        pltpu.make_async_remote_copy(
            src_ref=comb_send.at[ahead(k)], dst_ref=comb.at[me],
            send_sem=lse_sem.at[0], recv_sem=lse_sem.at[1],
            device_id={"cp": ahead(k)}, device_id_type=MESH,
        ).start()
        return carry

    lax.fori_loop(1, shards, lse_send, 0, unroll=True)

    for j in range(pairs):
        acc = acc_ref[j]
        out = acc[:HEAD_DIM] * (1.0 / acc[HEAD_DIM:HEAD_DIM + 1])
        for i in range(0, HEADS_STEP, 2):
            both = jnp.concatenate([out[:, i * rows:(i + 1) * rows], out[:, (i + 1) * rows:(i + 2) * rows]], axis=0).T
            at = (j * HEADS_STEP + i) * HEAD_DIM
            att_ref[:, at:at + 128] = both.astype(BF16)
    att_copy = pltpu.make_async_copy(att_ref, att_hbm, load_sem.at[0])
    att_copy.start()
    def lse_all():
        part = comb.at[pl.ds(0, shards - 1)]
        return pltpu.make_async_remote_copy(
            src_ref=part, dst_ref=part, send_sem=lse_sem.at[0], recv_sem=lse_sem.at[1],
            device_id={"cp": me}, device_id_type=MESH,
        )

    lse_all().wait_recv()

    got = comb[:, 0, :].T
    totals = jnp.sum(comb[:, 1, :], axis=0, keepdims=True)
    tw_ref[...] = flags * (float(dps * shards * rows) / totals)
    tw_move = pltpu.make_async_copy(tw_ref, tw_hbm, load_sem.at[2])
    tw_move.start()
    placed = None
    for r in range(block_rows):
        part = jnp.concatenate(pieces(got[r * heads:(r + 1) * heads]), axis=0)
        to = (iota((shards, rows), 1) == iota((shards, rows), 0) * block_rows + r).astype(F32).astype(BF16)
        more = jnp.dot(part, to, preferred_element_type=F32)
        placed = more if placed is None else placed + more
    lse_out_ref[...] = placed[:heads] + placed[heads:2 * heads] + placed[2 * heads:]
    lse_move = pltpu.make_async_copy(lse_out_ref, lse_hbm, load_sem.at[1])
    lse_move.start()

    for c in sends:
        c.wait_send()
    docs_all().wait_send()
    for t in range(2):
        for sem in range(2 * chips):
            slot_copy(t, back, 0, sem, me).wait_send()
    lse_all().wait_send()
    att_copy.wait()
    tw_move.wait()
    lse_move.wait()


def store(att_in, lse_in, tw_in, att_out, lse_out, tw_out, att, lse, tw, in_sem, out_sem):
    parts = 4
    step = att.shape[0] // parts
    moves = [(att_in.at[pl.ds(i * step, step)], att.at[pl.ds(i * step, step)], att_out.at[pl.ds(i * step, step)]) for i in range(parts)]
    moves += [(lse_in, lse, lse_out), (tw_in, tw, tw_out)]
    ins = [pltpu.make_async_copy(a, b, in_sem.at[i]) for i, (a, b, c) in enumerate(moves)]
    outs = [pltpu.make_async_copy(b, c, out_sem.at[i]) for i, (a, b, c) in enumerate(moves)]
    for c in ins:
        c.start()
    for i, c in enumerate(outs):
        ins[i].wait()
        c.start()
    for c in outs:
        c.wait()


def solution(mesh):
    dps, shards = mesh.shape["dp"], mesh.shape["cp"]
    half = HEAD_DIM // 2
    freq_np = np.broadcast_to(ROPE_BASE ** (-np.arange(half).astype(np.float64) / half)[:, None], (half, 128))

    def body(hidden, norm_gain, query_weight, keyval_weight, sink_logits, document_ids, block_owner, loss_mask):
        rows, width = hidden.shape[1:]
        heads = sink_logits.shape[0]
        kv_heads = keyval_weight.shape[1] // (2 * HEAD_DIM)
        qdim = heads * HEAD_DIM
        back = DOC_MOST // rows
        slots = back + 1
        pairs = heads // HEADS_STEP
        widest = 3 * rows
        shape = (rows, width, heads, kv_heads, shards, dps)
        hbm = pl.BlockSpec(memory_space=pltpu.HBM)
        dma = pltpu.SemaphoreType.DMA
        att, lse, tw = pl.pallas_call(
            functools.partial(kernel, shape),
            name="attention_step",
            out_shape=(
                jax.ShapeDtypeStruct((rows, qdim), BF16),
                jax.ShapeDtypeStruct((heads, rows), F32),
                jax.ShapeDtypeStruct((1, rows), F32),
            ),
            in_specs=[hbm] * 9,
            out_specs=(hbm, hbm, hbm),
            scratch_shapes=[
                pltpu.VMEM((width, rows), BF16),
                pltpu.VMEM((width,), F32),
                pltpu.VMEM((width, keyval_weight.shape[1]), BF16),
                pltpu.VMEM((qdim // Q_CHUNK, width, Q_CHUNK), BF16),
                pltpu.VMEM((rows, width), BF16),
                pltpu.VMEM((qdim, rows), F32),
                pltpu.VMEM((pairs, 128, HEADS_STEP * rows), BF16),
                pltpu.VMEM((slots, kv_heads // 2, rows, 128), BF16),
                pltpu.VMEM((slots, kv_heads, HEAD_DIM, rows), BF16),
                pltpu.VMEM((slots, rows, rows), F32),
                pltpu.VMEM((slots, 1, rows), jnp.int32),
                pltpu.VMEM((1, 1, rows), F32),
                pltpu.VMEM((dps, 1, rows), F32),
                pltpu.VMEM((pairs, 8, HEADS_STEP * rows), F32),
                pltpu.VMEM((pairs, HEAD_DIM + 16, HEADS_STEP * rows), F32),
                pltpu.VMEM((heads, rows), F32),
                pltpu.VMEM((shards, 2, rows), F32),
                pltpu.VMEM((shards, 2, rows), F32),
                pltpu.VMEM((widest, HEADS_STEP * rows), F32),
                pltpu.VMEM((widest, HEADS_STEP * rows), F32),
                pltpu.VMEM((8, HEADS_STEP * rows), F32),
                pltpu.VMEM((8, HEADS_STEP * rows), F32),
                pltpu.VMEM((shards, 3 * rows), BF16),
                pltpu.SMEM((heads,), F32),
                pltpu.VMEM((1, shards), jnp.int32),
                pltpu.VMEM((1, rows), jnp.int32),
                pltpu.VMEM((half, 128), F32),
                pltpu.VMEM((rows, qdim), BF16),
                pltpu.VMEM((heads, rows), F32),
                pltpu.VMEM((1, rows), F32),
                dma((8,)), dma((qdim // Q_CHUNK,)),
                dma((2,)),
                dma((2, back)), dma((2, back)),
                dma((dps - 1,)), dma((dps - 1,)),
                dma((2,)),
            ],
            compiler_params=pltpu.CompilerParams(
                collective_id=0, has_side_effects=True, vmem_limit_bytes=58 * 1024 * 1024
            ),
        )(
            hidden[0].T, norm_gain, query_weight, keyval_weight, sink_logits,
            document_ids, block_owner[0], loss_mask,
            jnp.asarray(freq_np, F32),
        )
        results = (att, lse, tw)
        att, lse, tw = pl.pallas_call(
            store,
            name="store_results",
            out_shape=tuple(jax.ShapeDtypeStruct(r.shape, r.dtype) for r in results),
            in_specs=[hbm] * 3,
            out_specs=(hbm,) * 3,
            scratch_shapes=[pltpu.VMEM(r.shape, r.dtype) for r in results] + [dma((6,)), dma((6,))],
            compiler_params=pltpu.CompilerParams(vmem_limit_bytes=58 * 1024 * 1024),
        )(*results)
        return att[None], lse[None], tw

    return jax.shard_map(
        body,
        mesh=mesh,
        in_specs=(
            P("dp", "cp", None), P(), P(), P(), P(), P("dp", "cp"), P("dp", "cp", None), P("dp", "cp"),
        ),
        out_specs=(P("dp", "cp", None), P("dp", None, "cp"), P("dp", "cp")),
        check_vma=False,
    )
```

```python
import functools
import math

import jax
import jax.numpy as jnp
import numpy as np
from jax import lax
from jax.experimental import pallas as pl
from jax.experimental.pallas import tpu as pltpu
from jax.sharding import PartitionSpec as P

MESH = pl.DeviceIdType.MESH
HEAD_DIM = 64
DOC_MOST = 1024
ROPE_BASE = 150000.0
NORM_EPS = 1e-05
MASKED = -1e30
LOG2E = 1.4426950408889634
LN2 = 0.6931471805599453
F32 = jnp.float32
BF16 = jnp.bfloat16
NT = (((1,), (1,)), ((), ()))
Q_CHUNK = 512
HEADS_STEP = 8
DOC_AT = 3
HOOK_0, HOOK_1, HOOK_2 = 2, 2, 0


def iota(shape, dim):
    return lax.broadcasted_iota(jnp.int32, shape, dim)


def exact_dot(a, b, dims=(((1,), (0,)), ((), ()))):
    return lax.dot_general(a, b, dims, precision=lax.Precision.HIGHEST, preferred_element_type=F32)


def cos_sin(angle):
    k = jnp.floor(angle * (2.0 / math.pi) + 0.5)
    r = ((angle - k * 1.5703125) - k * 4.837512969970703125e-4) - k * 7.549789954891882e-8
    z = r * r
    s = ((-1.9515295891e-4 * z + 8.3321608736e-3) * z - 1.6666654611e-1) * z * r + r
    c = ((2.443315711809948e-5 * z - 1.388731625493765e-3) * z + 4.166664568298827e-2) * z * z - 0.5 * z + 1.0
    q = k.astype(jnp.int32) & 3
    odd = (q & 1) == 1
    cosine = jnp.where(odd, s, c)
    sine = jnp.where(odd, c, s)
    cosine = jnp.where((q == 1) | (q == 2), -cosine, cosine)
    sine = jnp.where(q >= 2, -sine, sine)
    return cosine, sine


def kernel(
    shape,
    hidden_hbm, gain_hbm, qw_hbm, kvw_hbm, sink_hbm, docs_hbm, owner_hbm, mask_hbm, freq_hbm,
    att_hbm, lse_hbm, tw_hbm,
    hid, gain, kvw, qw, normed, qt, qz, kbuf, vbuf, bias,
    docs_buf, cnt_send, cnt_buf, m_ref, acc_ref, lse_ref, comb_send, comb, s_even, s_odd, top_even, top_odd,
    chosen3, sink_ref, owner_ref, mask_ref, freq_ref, att_ref, lse_out_ref, tw_ref,
    load_sem, qw_sem,
    doc_sem, kv_ssem, kv_rsem, cnt_ssem, cnt_rsem, lse_sem,
):
    rows, width, heads, kv_heads, shards, dps = shape
    back = DOC_MOST // rows
    per_kv = heads // kv_heads
    block_rows = rows // shards
    me = lax.axis_index("cp")
    my_dp = lax.axis_index("dp")
    qdim = heads * HEAD_DIM
    n_chunks = qdim // Q_CHUNK
    pairs = heads // HEADS_STEP
    half = HEAD_DIM // 2

    def ahead(k):
        return lax.rem(me + k, shards)

    loads = [
        pltpu.make_async_copy(hidden_hbm, hid, load_sem.at[0]),
        pltpu.make_async_copy(gain_hbm, gain, load_sem.at[1]),
        pltpu.make_async_copy(docs_hbm, docs_buf.at[back], load_sem.at[2]),
        pltpu.make_async_copy(mask_hbm, mask_ref, load_sem.at[3]),
        pltpu.make_async_copy(kvw_hbm, kvw, load_sem.at[4]),
        pltpu.make_async_copy(freq_hbm, freq_ref, load_sem.at[5]),
        pltpu.make_async_copy(sink_hbm, sink_ref, load_sem.at[6]),
        pltpu.make_async_copy(owner_hbm, owner_ref, load_sem.at[7]),
    ]
    for c in loads:
        c.start()

    barrier = pltpu.get_barrier_semaphore()

    for k in range(1, back + 1):
        for at in (k, shards - k):
            pl.semaphore_signal(barrier, inc=1, device_id={"cp": ahead(at)}, device_id_type=MESH)
    for k in range(1, dps):
        pl.semaphore_signal(
            barrier, inc=1, device_id={"dp": lax.rem(my_dp + k, dps)}, device_id_type=MESH
        )

    loads[0].wait()
    loads[1].wait()
    q_loads = [
        pltpu.make_async_copy(qw_hbm.at[:, pl.ds(i * Q_CHUNK, Q_CHUNK)], qw.at[i], qw_sem.at[i])
        for i in range(n_chunks)
    ]
    for c in q_loads:
        c.start()
    loads[2].wait()
    loads[3].wait()
    own_docs = docs_buf[back]
    flags = mask_ref[...].astype(F32)
    cnt_row = jnp.broadcast_to(jnp.sum(flags, axis=1, keepdims=True), (1, rows))
    cnt_send[0] = cnt_row
    cnt_buf[0] = cnt_row
    x = hid[...].T.astype(F32)
    inv = lax.rsqrt(jnp.sum(x * x, axis=1, keepdims=True) * (1.0 / width) + NORM_EPS)
    normed[...] = (x * inv * gain[...].reshape(1, width)).astype(BF16)

    pl.semaphore_wait(barrier, 2 * back + dps - 1)

    sends = []

    def send(src, dst, ssem, rsem, device, keep=True):
        c = pltpu.make_async_remote_copy(
            src_ref=src, dst_ref=dst, send_sem=ssem, recv_sem=rsem,
            device_id=device, device_id_type=MESH,
        )
        c.start()
        if keep:
            sends.append(c)
        return c

    for k in range(1, back + 1):
        send(docs_buf.at[back], docs_buf.at[back - k], doc_sem.at[0], doc_sem.at[1], {"cp": ahead(k)}, False)
    cnt_copies = []
    for k in range(1, dps):
        cnt_copies.append(send(
            cnt_send.at[0], cnt_buf.at[k], cnt_ssem.at[k - 1], cnt_rsem.at[k - 1],
            {"dp": lax.rem(my_dp + k, dps)},
        ))

    core = lax.rem(me, 2)
    chips = back // 2
    z = lax.rem(me // 2, chips)
    corner = me - 2 * z
    pieces_v, pieces_k = (0, 1), (2, 3)

    def piece(t, slot):
        if t < 2:
            return vbuf.at[slot, pl.ds(t * (kv_heads // 2), kv_heads // 2)]
        return kbuf.at[slot, t - 2]

    def slot_copy(t, src, dst, sem, device):
        return pltpu.make_async_remote_copy(
            src_ref=piece(t, src), dst_ref=piece(t, dst), send_sem=kv_ssem.at[t, sem],
            recv_sem=kv_rsem.at[t, dst], device_id={"cp": device}, device_id_type=MESH,
        )

    def row_copy(t, k, src):
        return slot_copy(t, src, back - 2 * k, k, corner + 2 * lax.rem(z + k, chips))

    def next_row_copy(t):
        return slot_copy(t, back, 0, 0, ahead(back))

    def partner_copy(t, src, dst):
        return slot_copy(t, src, dst, chips + (src // 2) % chips, me + 1 - 2 * core)

    def send_own(t):
        @pl.when(core == 0)
        def _():
            partner_copy(t, back, back - 1).start()

        next_row_copy(t).start()
        for k in (3, 1):
            @pl.when(z + k < chips)
            def _(k=k):
                row_copy(t, k, back).start()

        slot_copy(t, back, back // 2, 2, ahead(back // 2)).start()

    def arrived(t, slot):
        slot_copy(t, slot, slot, 0, me).wait_recv()

    def serve(t, slot):
        arrived(t, slot)
        if isinstance(slot, int) and slot == 0:
            for k in (3, 1):
                @pl.when(z + k >= chips)
                def _(k=k):
                    row_copy(t, k, 0).start()

            @pl.when(core == 1)
            def _():
                partner_copy(t, 0, 1).start()
        else:
            partner_copy(t, slot, slot - 1 + 2 * core).start()

    loads[4].wait()
    kv = jnp.dot(normed[...], kvw[...], preferred_element_type=F32)
    kv_width = kv_heads * HEAD_DIM
    raw_kt = []
    for t in range(kv_heads // 2):
        v_t = kv[:, kv_width + t * 128:kv_width + (t + 1) * 128].T.astype(BF16)
        vbuf[back, 2 * t] = v_t[:HEAD_DIM]
        vbuf[back, 2 * t + 1] = v_t[HEAD_DIM:]
        raw_kt.append(kv[:, t * 128:(t + 1) * 128].T)

    def q_part(i):
        q_loads[i].wait()
        part = jnp.dot(normed[...], qw[i], preferred_element_type=F32)
        for t in range(Q_CHUNK // 128):
            at = i * Q_CHUNK + t * 128
            qt[at:at + 128] = part[:, t * 128:(t + 1) * 128].T

    for t in pieces_v:
        send_own(t)

    def docs_all():
        part = docs_buf.at[pl.ds(0, back)]
        return pltpu.make_async_remote_copy(
            src_ref=part, dst_ref=part, send_sem=doc_sem.at[0], recv_sem=doc_sem.at[1],
            device_id={"cp": me}, device_id_type=MESH,
        )

    for i in range(DOC_AT):
        q_part(i)

    for i in range(5, 8):
        loads[i].wait()
    spread = (iota((shards, rows), 1) // block_rows == iota((shards, rows), 0)).astype(F32)
    owner_row = jnp.broadcast_to(owner_ref[...].astype(F32), (8, shards))
    owner_wide = exact_dot(owner_row, spread)[:1]
    chosen = jnp.broadcast_to(owner_wide, (shards, rows)) == iota((shards, rows), 0).astype(F32)
    chosen = chosen.astype(F32).astype(BF16)
    chosen3[...] = jnp.concatenate([chosen] * 3, axis=1)

    docs_all().wait_recv()
    square = (rows, 128)
    lane = iota(square, 1)
    sub = iota(square, 0)
    own_row = jnp.broadcast_to(own_docs.astype(F32), square)
    own_col = own_row.T
    count = jnp.zeros(square, F32)
    for b in range(back + 1):
        window_docs = docs_buf[b].astype(F32)
        if b < back:
            window_docs = jnp.where(me >= back - b, window_docs, -1.0)
        count = count + (jnp.broadcast_to(window_docs, square) < own_col).astype(F32)
    start_row = jnp.broadcast_to(jnp.sum(count, axis=1, keepdims=True), square).T
    within = (lane[:half] + back * rows).astype(F32) - start_row[:half]
    cosine, sine = cos_sin(within * freq_ref[...])

    def rope(u):
        a, b = u[:half], u[half:]
        return jnp.concatenate([a * cosine - b * sine, b * cosine + a * sine], axis=0)

    for t in range(kv_heads // 2):
        u = raw_kt[t]
        u = jnp.concatenate([rope(u[:HEAD_DIM]), rope(u[HEAD_DIM:])], axis=0)
        kbuf[back, t] = u.T.astype(BF16)
    for t in pieces_k:
        send_own(t)

    for t in pieces_v:
        serve(t, 0)
    for i in range(DOC_AT, n_chunks):
        q_part(i)

    scale = HEAD_DIM ** (-0.5)
    zeros = jnp.zeros((HEAD_DIM, rows), BF16)
    for h in range(heads):
        y = (rope(qt[h * HEAD_DIM:(h + 1) * HEAD_DIM]) * scale).astype(BF16)
        at = (h // per_kv) % 2
        lanes = slice((h % HEADS_STEP) * rows, (h % HEADS_STEP + 1) * rows)
        qz[h // HEADS_STEP, at * HEAD_DIM:(at + 1) * HEAD_DIM, lanes] = y
        qz[h // HEADS_STEP, (1 - at) * HEAD_DIM:(2 - at) * HEAD_DIM, lanes] = zeros

    for b in range(back + 1):
        place = (sub + b * rows).astype(F32)
        allowed = place >= start_row
        if b == back:
            allowed = allowed & (sub <= lane)
        bias[b] = jnp.where(allowed, 0.0, MASKED)

    extra = 1 + 6 * core
    front = (3 - z) // 3
    one = 6 - 2 * front
    three = 2 + 4 * front
    two_ = 12 - one - three

    def odd(slot):
        return slot + 1 - 2 * core

    def serve_all(slot):
        for t in pieces_v + pieces_k:
            serve(t, slot)

    def wait_all(slot):
        for t in pieces_v + pieces_k:
            arrived(t, slot)

    def serve_next_row():
        for t in pieces_k:
            serve(t, 0)

    def before_first():
        serve_next_row()

        @pl.when(z > 0)
        def _():
            serve_all(one)

        wait_all(extra)

    def serve_first():
        @pl.when(z == 0)
        def _():
            serve_all(one)

    groups = (
        ((back,), lambda: None, -1, None),
        ((0, extra), before_first, HOOK_0, serve_first),
        ((one, odd(one)), lambda: wait_all(odd(one)), HOOK_1, lambda: serve_all(two_)),
        ((two_, odd(two_)), lambda: wait_all(odd(two_)), HOOK_2, lambda: serve_all(three)),
        ((three, odd(three)), lambda: wait_all(odd(three)), -1, None),
    )
    two = HEADS_STEP * rows
    head_lane = iota((1, two), 1) // rows
    acc_rows = HEAD_DIM + 16
    for gi, (slots, before, hook_at, hook) in enumerate(groups):
        with jax.named_scope("before%d" % gi):
            before()
        first, last = gi == 0, gi == len(groups) - 1
        nb = len(slots)
        ones_rows = jnp.ones((16, nb * rows), BF16)

        def score(j, s_ref, t_ref, slots=slots, nb=nb):
            a = j // (per_kv // HEADS_STEP)
            kb = jnp.concatenate([kbuf[b, a // 2] for b in slots], axis=0)
            s = jnp.dot(kb, qz[j], preferred_element_type=F32)
            top = None
            for b in range(nb):
                bb = bias[slots[b]]
                sb = s[b * rows:(b + 1) * rows] * LOG2E + jnp.concatenate([bb] * HEADS_STEP, axis=1)
                s_ref[b * rows:(b + 1) * rows] = sb
                part = jnp.max(sb.reshape(rows // 8, 8, two), axis=0)
                top = part if top is None else jnp.maximum(top, part)
            t_ref[...] = top

        def mix(j, s_ref, t_ref, slots=slots, nb=nb, first=first, last=last, ones_rows=ones_rows):
            a = j // (per_kv // HEADS_STEP)
            top = jnp.max(t_ref[...], axis=0, keepdims=True)
            if first:
                old = jnp.zeros((1, two), F32)
                for i in range(HEADS_STEP):
                    old = jnp.where(head_lane == i, sink_ref[HEADS_STEP * j + i] * LOG2E, old)
            else:
                old = m_ref[j][:1]
            new = jnp.maximum(old, top)
            mixed = None
            for b in range(0, nb, 2):
                part = slots[b:b + 2]
                n = len(part) * rows
                weights = jnp.exp2(s_ref[b * rows:b * rows + n] - new).astype(BF16)
                vt = jnp.concatenate([vbuf[i, a] for i in part], axis=1)
                vt = jnp.concatenate([vt, ones_rows[:, :n]], axis=0)
                more = jnp.dot(vt, weights, preferred_element_type=F32)
                mixed = more if mixed is None else mixed + more
            shrink = jnp.exp2(old - new)
            if first:
                acc = mixed + jnp.where(iota((acc_rows, two), 0) >= HEAD_DIM, shrink, 0.0)
            else:
                acc = acc_ref[j] * shrink + mixed
            if last:
                total = acc[HEAD_DIM:HEAD_DIM + 1]
                acc_ref[j] = acc
                lse = (new + jnp.log2(total)) * LN2
                for i in range(HEADS_STEP):
                    lse_ref[pl.ds(HEADS_STEP * j + i, 1), :] = lse[:, i * rows:(i + 1) * rows]
            else:
                acc_ref[j] = acc
                m_ref[j] = jnp.broadcast_to(new, (8, two))

        def two_pairs(i, carry, score=score, mix=mix):
            j = 2 * i
            score(j + 1, s_odd, top_odd)
            mix(j, s_even, top_even)
            score(lax.rem(j + 2, pairs), s_even, top_even)
            mix(j + 1, s_odd, top_odd)
            return carry

        with jax.named_scope("loop%d" % gi):
            score(0, s_even, top_even)
            for j in range(0, pairs, 2):
                if j == hook_at:
                    with jax.named_scope("hook%d" % gi):
                        hook()
                score(j + 1, s_odd, top_odd)
                mix(j, s_even, top_even)
                if j + 2 < pairs:
                    score(j + 2, s_even, top_even)
                mix(j + 1, s_odd, top_odd)

    for c in cnt_copies:
        c.wait_recv()
    cnt = cnt_buf[0]
    for k in range(1, dps):
        cnt = cnt + cnt_buf[k]

    def pieces(v):
        hi = v.astype(BF16)
        rest = v - hi.astype(F32)
        mid = rest.astype(BF16)
        return [hi, mid, (rest - mid.astype(F32)).astype(BF16)]

    wide = block_rows * heads
    lse4 = jnp.concatenate([lse_ref[...]] * block_rows, axis=0)
    lse4 = jnp.where(iota((wide, rows), 1) % block_rows == iota((wide, rows), 0) // heads, lse4, 0.0)
    lse4 = jnp.concatenate(pieces(lse4), axis=1)
    comb_send[:, 0, :] = lax.dot_general(chosen3[...], lse4, NT, preferred_element_type=F32)
    comb_send[:, 1, :] = jnp.broadcast_to(cnt, (shards, rows))
    comb[me] = comb_send[me]

    def lse_send(k, carry):
        pltpu.make_async_remote_copy(
            src_ref=comb_send.at[ahead(k)], dst_ref=comb.at[me],
            send_sem=lse_sem.at[0], recv_sem=lse_sem.at[1],
            device_id={"cp": ahead(k)}, device_id_type=MESH,
        ).start()
        return carry

    lax.fori_loop(1, shards, lse_send, 0, unroll=True)

    for j in range(pairs):
        acc = acc_ref[j]
        out = acc[:HEAD_DIM] * (1.0 / acc[HEAD_DIM:HEAD_DIM + 1])
        for i in range(0, HEADS_STEP, 2):
            both = jnp.concatenate([out[:, i * rows:(i + 1) * rows], out[:, (i + 1) * rows:(i + 2) * rows]], axis=0).T
            at = (j * HEADS_STEP + i) * HEAD_DIM
            att_ref[:, at:at + 128] = both.astype(BF16)
    att_copy = pltpu.make_async_copy(att_ref, att_hbm, load_sem.at[0])
    att_copy.start()
    def lse_all():
        part = comb.at[pl.ds(0, shards - 1)]
        return pltpu.make_async_remote_copy(
            src_ref=part, dst_ref=part, send_sem=lse_sem.at[0], recv_sem=lse_sem.at[1],
            device_id={"cp": me}, device_id_type=MESH,
        )

    lse_all().wait_recv()

    got = comb[:, 0, :].T
    totals = jnp.sum(comb[:, 1, :], axis=0, keepdims=True)
    tw_ref[...] = flags * (float(dps * shards * rows) / totals)
    tw_move = pltpu.make_async_copy(tw_ref, tw_hbm, load_sem.at[2])
    tw_move.start()
    placed = None
    for r in range(block_rows):
        part = jnp.concatenate(pieces(got[r * heads:(r + 1) * heads]), axis=0)
        to = (iota((shards, rows), 1) == iota((shards, rows), 0) * block_rows + r).astype(F32).astype(BF16)
        more = jnp.dot(part, to, preferred_element_type=F32)
        placed = more if placed is None else placed + more
    lse_out_ref[...] = placed[:heads] + placed[heads:2 * heads] + placed[2 * heads:]
    lse_move = pltpu.make_async_copy(lse_out_ref, lse_hbm, load_sem.at[1])
    lse_move.start()

    for c in sends:
        c.wait_send()
    docs_all().wait_send()
    for t in range(4):
        for sem in range(2 * chips):
            slot_copy(t, back, 0, sem, me).wait_send()
    lse_all().wait_send()
    att_copy.wait()
    tw_move.wait()
    lse_move.wait()


def store(att_in, lse_in, tw_in, att_out, lse_out, tw_out, att, lse, tw, in_sem, out_sem):
    parts = 4
    step = att.shape[0] // parts
    moves = [(att_in.at[pl.ds(i * step, step)], att.at[pl.ds(i * step, step)], att_out.at[pl.ds(i * step, step)]) for i in range(parts)]
    moves += [(lse_in, lse, lse_out), (tw_in, tw, tw_out)]
    ins = [pltpu.make_async_copy(a, b, in_sem.at[i]) for i, (a, b, c) in enumerate(moves)]
    outs = [pltpu.make_async_copy(b, c, out_sem.at[i]) for i, (a, b, c) in enumerate(moves)]
    for c in ins:
        c.start()
    for i, c in enumerate(outs):
        ins[i].wait()
        c.start()
    for c in outs:
        c.wait()


def solution(mesh):
    dps, shards = mesh.shape["dp"], mesh.shape["cp"]
    half = HEAD_DIM // 2
    freq_np = np.broadcast_to(ROPE_BASE ** (-np.arange(half).astype(np.float64) / half)[:, None], (half, 128))

    def body(hidden, norm_gain, query_weight, keyval_weight, sink_logits, document_ids, block_owner, loss_mask):
        rows, width = hidden.shape[1:]
        heads = sink_logits.shape[0]
        kv_heads = keyval_weight.shape[1] // (2 * HEAD_DIM)
        qdim = heads * HEAD_DIM
        back = DOC_MOST // rows
        slots = back + 1
        pairs = heads // HEADS_STEP
        widest = 2 * rows
        shape = (rows, width, heads, kv_heads, shards, dps)
        hbm = pl.BlockSpec(memory_space=pltpu.HBM)
        dma = pltpu.SemaphoreType.DMA
        att, lse, tw = pl.pallas_call(
            functools.partial(kernel, shape),
            name="attention_step",
            out_shape=(
                jax.ShapeDtypeStruct((rows, qdim), BF16),
                jax.ShapeDtypeStruct((heads, rows), F32),
                jax.ShapeDtypeStruct((1, rows), F32),
            ),
            in_specs=[hbm] * 9,
            out_specs=(hbm, hbm, hbm),
            scratch_shapes=[
                pltpu.VMEM((width, rows), BF16),
                pltpu.VMEM((width,), F32),
                pltpu.VMEM((width, keyval_weight.shape[1]), BF16),
                pltpu.VMEM((qdim // Q_CHUNK, width, Q_CHUNK), BF16),
                pltpu.VMEM((rows, width), BF16),
                pltpu.VMEM((qdim, rows), F32),
                pltpu.VMEM((pairs, 128, HEADS_STEP * rows), BF16),
                pltpu.VMEM((slots, kv_heads // 2, rows, 128), BF16),
                pltpu.VMEM((slots, kv_heads, HEAD_DIM, rows), BF16),
                pltpu.VMEM((slots, rows, rows), F32),
                pltpu.VMEM((slots, 1, rows), jnp.int32),
                pltpu.VMEM((1, 1, rows), F32),
                pltpu.VMEM((dps, 1, rows), F32),
                pltpu.VMEM((pairs, 8, HEADS_STEP * rows), F32),
                pltpu.VMEM((pairs, HEAD_DIM + 16, HEADS_STEP * rows), F32),
                pltpu.VMEM((heads, rows), F32),
                pltpu.VMEM((shards, 2, rows), F32),
                pltpu.VMEM((shards, 2, rows), F32),
                pltpu.VMEM((widest, HEADS_STEP * rows), F32),
                pltpu.VMEM((widest, HEADS_STEP * rows), F32),
                pltpu.VMEM((8, HEADS_STEP * rows), F32),
                pltpu.VMEM((8, HEADS_STEP * rows), F32),
                pltpu.VMEM((shards, 3 * rows), BF16),
                pltpu.SMEM((heads,), F32),
                pltpu.VMEM((1, shards), jnp.int32),
                pltpu.VMEM((1, rows), jnp.int32),
                pltpu.VMEM((half, 128), F32),
                pltpu.VMEM((rows, qdim), BF16),
                pltpu.VMEM((heads, rows), F32),
                pltpu.VMEM((1, rows), F32),
                dma((8,)), dma((qdim // Q_CHUNK,)),
                dma((2,)),
                dma((4, back)), dma((4, back)),
                dma((dps - 1,)), dma((dps - 1,)),
                dma((2,)),
            ],
            compiler_params=pltpu.CompilerParams(
                collective_id=0, has_side_effects=True, vmem_limit_bytes=58 * 1024 * 1024
            ),
        )(
            hidden[0].T, norm_gain, query_weight, keyval_weight, sink_logits,
            document_ids, block_owner[0], loss_mask,
            jnp.asarray(freq_np, F32),
        )
        results = (att, lse, tw)
        att, lse, tw = pl.pallas_call(
            store,
            name="store_results",
            out_shape=tuple(jax.ShapeDtypeStruct(r.shape, r.dtype) for r in results),
            in_specs=[hbm] * 3,
            out_specs=(hbm,) * 3,
            scratch_shapes=[pltpu.VMEM(r.shape, r.dtype) for r in results] + [dma((6,)), dma((6,))],
            compiler_params=pltpu.CompilerParams(vmem_limit_bytes=58 * 1024 * 1024),
        )(*results)
        return att[None], lse[None], tw

    return jax.shard_map(
        body,
        mesh=mesh,
        in_specs=(
            P("dp", "cp", None), P(), P(), P(), P(), P("dp", "cp"), P("dp", "cp", None), P("dp", "cp"),
        ),
        out_specs=(P("dp", "cp", None), P("dp", None, "cp"), P("dp", "cp")),
        check_vma=False,
    )
```

```python
import functools
import math

import jax
import jax.numpy as jnp
import numpy as np
from jax import lax
from jax.experimental import pallas as pl
from jax.experimental.pallas import tpu as pltpu
from jax.sharding import PartitionSpec as P

MESH = pl.DeviceIdType.MESH
HEAD_DIM = 64
DOC_MOST = 1024
ROPE_BASE = 150000.0
NORM_EPS = 1e-05
MASKED = -1e30
LOG2E = 1.4426950408889634
LN2 = 0.6931471805599453
F32 = jnp.float32
BF16 = jnp.bfloat16
NT = (((1,), (1,)), ((), ()))
Q_CHUNK = 512
HEADS_STEP = 8
DOC_AT = 3
HOOK_0, HOOK_1 = 2, 2


def iota(shape, dim):
    return lax.broadcasted_iota(jnp.int32, shape, dim)


def exact_dot(a, b, dims=(((1,), (0,)), ((), ()))):
    return lax.dot_general(a, b, dims, precision=lax.Precision.HIGHEST, preferred_element_type=F32)


def cos_sin(angle):
    k = jnp.floor(angle * (2.0 / math.pi) + 0.5)
    r = ((angle - k * 1.5703125) - k * 4.837512969970703125e-4) - k * 7.549789954891882e-8
    z = r * r
    s = ((-1.9515295891e-4 * z + 8.3321608736e-3) * z - 1.6666654611e-1) * z * r + r
    c = ((2.443315711809948e-5 * z - 1.388731625493765e-3) * z + 4.166664568298827e-2) * z * z - 0.5 * z + 1.0
    q = k.astype(jnp.int32) & 3
    odd = (q & 1) == 1
    cosine = jnp.where(odd, s, c)
    sine = jnp.where(odd, c, s)
    cosine = jnp.where((q == 1) | (q == 2), -cosine, cosine)
    sine = jnp.where(q >= 2, -sine, sine)
    return cosine, sine


def kernel(
    shape,
    hidden_hbm, gain_hbm, qw_hbm, kvw_hbm, sink_hbm, docs_hbm, owner_hbm, mask_hbm, freq_hbm,
    att_hbm, lse_hbm, tw_hbm,
    hid, gain, kvw, qw, normed, qt, qz, kbuf, vbuf, bias,
    docs_buf, cnt_send, cnt_buf, m_ref, acc_ref, lse_ref, comb_send, comb, s_even, s_odd, top_even, top_odd,
    chosen3, sink_ref, owner_ref, mask_ref, freq_ref, att_ref, lse_out_ref, tw_ref,
    load_sem, qw_sem,
    doc_sem, kv_ssem, kv_rsem, cnt_ssem, cnt_rsem, lse_sem,
):
    rows, width, heads, kv_heads, shards, dps = shape
    back = DOC_MOST // rows
    per_kv = heads // kv_heads
    block_rows = rows // shards
    me = lax.axis_index("cp")
    my_dp = lax.axis_index("dp")
    qdim = heads * HEAD_DIM
    n_chunks = qdim // Q_CHUNK
    pairs = heads // HEADS_STEP
    half = HEAD_DIM // 2

    def ahead(k):
        return lax.rem(me + k, shards)

    loads = [
        pltpu.make_async_copy(hidden_hbm, hid, load_sem.at[0]),
        pltpu.make_async_copy(gain_hbm, gain, load_sem.at[1]),
        pltpu.make_async_copy(docs_hbm, docs_buf.at[back], load_sem.at[2]),
        pltpu.make_async_copy(mask_hbm, mask_ref, load_sem.at[3]),
        pltpu.make_async_copy(kvw_hbm, kvw, load_sem.at[4]),
        pltpu.make_async_copy(freq_hbm, freq_ref, load_sem.at[5]),
        pltpu.make_async_copy(sink_hbm, sink_ref, load_sem.at[6]),
        pltpu.make_async_copy(owner_hbm, owner_ref, load_sem.at[7]),
    ]
    for c in loads:
        c.start()

    barrier = pltpu.get_barrier_semaphore()

    for k in range(1, back + 1):
        for at in (k, shards - k):
            pl.semaphore_signal(barrier, inc=1, device_id={"cp": ahead(at)}, device_id_type=MESH)
    for k in range(1, dps):
        pl.semaphore_signal(
            barrier, inc=1, device_id={"dp": lax.rem(my_dp + k, dps)}, device_id_type=MESH
        )

    loads[0].wait()
    loads[1].wait()
    q_loads = [
        pltpu.make_async_copy(qw_hbm.at[:, pl.ds(i * Q_CHUNK, Q_CHUNK)], qw.at[i], qw_sem.at[i])
        for i in range(n_chunks)
    ]
    for c in q_loads:
        c.start()
    loads[2].wait()
    loads[3].wait()
    own_docs = docs_buf[back]
    flags = mask_ref[...].astype(F32)
    cnt_row = jnp.broadcast_to(jnp.sum(flags, axis=1, keepdims=True), (1, rows))
    cnt_send[0] = cnt_row
    cnt_buf[0] = cnt_row
    x = hid[...].T.astype(F32)
    inv = lax.rsqrt(jnp.sum(x * x, axis=1, keepdims=True) * (1.0 / width) + NORM_EPS)
    normed[...] = (x * inv * gain[...].reshape(1, width)).astype(BF16)

    pl.semaphore_wait(barrier, 2 * back + dps - 1)

    sends = []

    def send(src, dst, ssem, rsem, device, keep=True):
        c = pltpu.make_async_remote_copy(
            src_ref=src, dst_ref=dst, send_sem=ssem, recv_sem=rsem,
            device_id=device, device_id_type=MESH,
        )
        c.start()
        if keep:
            sends.append(c)
        return c

    for k in range(1, back + 1):
        send(docs_buf.at[back], docs_buf.at[back - k], doc_sem.at[0], doc_sem.at[1], {"cp": ahead(k)}, False)
    cnt_copies = []
    for k in range(1, dps):
        cnt_copies.append(send(
            cnt_send.at[0], cnt_buf.at[k], cnt_ssem.at[k - 1], cnt_rsem.at[k - 1],
            {"dp": lax.rem(my_dp + k, dps)},
        ))

    core = lax.rem(me, 2)
    chips = back // 2
    z = lax.rem(me // 2, chips)
    corner = me - 2 * z
    pieces_v, pieces_k = (0, 1), (2, 3)

    def piece(t, slot):
        if t < 2:
            return vbuf.at[slot, pl.ds(t * (kv_heads // 2), kv_heads // 2)]
        return kbuf.at[slot, t - 2]

    def slot_copy(t, src, dst, sem, device):
        return pltpu.make_async_remote_copy(
            src_ref=piece(t, src), dst_ref=piece(t, dst), send_sem=kv_ssem.at[t, sem],
            recv_sem=kv_rsem.at[t, dst], device_id={"cp": device}, device_id_type=MESH,
        )

    def row_copy(t, k, src):
        return slot_copy(t, src, back - 2 * k, k, corner + 2 * lax.rem(z + k, chips))

    def next_row_copy(t):
        return slot_copy(t, back, 0, 0, ahead(back))

    def partner_copy(t, src, dst):
        return slot_copy(t, src, dst, chips + (src // 2) % chips, me + 1 - 2 * core)

    def send_own(t):
        @pl.when(core == 0)
        def _():
            partner_copy(t, back, back - 1).start()

        next_row_copy(t).start()
        @pl.when(z == 0)
        def _():
            row_copy(t, 3, back).start()

        @pl.when(z < chips - 1)
        def _():
            row_copy(t, 1, back).start()

    def send_two(t):
        @pl.when(z == 1)
        def _():
            slot_copy(t, back, back - 6, 3, ahead(6)).start()

        slot_copy(t, back, back // 2, 2, ahead(back // 2)).start()

    def arrived(t, slot):
        slot_copy(t, slot, slot, 0, me).wait_recv()

    def serve(t, slot):
        arrived(t, slot)
        if isinstance(slot, int) and slot == 0:
            @pl.when(z > 1)
            def _():
                row_copy(t, 3, 0).start()

            @pl.when(z == chips - 1)
            def _():
                row_copy(t, 1, 0).start()

            @pl.when(core == 1)
            def _():
                partner_copy(t, 0, 1).start()
        else:
            partner_copy(t, slot, slot - 1 + 2 * core).start()

    loads[4].wait()
    kv = jnp.dot(normed[...], kvw[...], preferred_element_type=F32)
    kv_width = kv_heads * HEAD_DIM
    raw_kt = []
    for t in range(kv_heads // 2):
        v_t = kv[:, kv_width + t * 128:kv_width + (t + 1) * 128].T.astype(BF16)
        vbuf[back, 2 * t] = v_t[:HEAD_DIM]
        vbuf[back, 2 * t + 1] = v_t[HEAD_DIM:]
        raw_kt.append(kv[:, t * 128:(t + 1) * 128].T)

    def q_part(i):
        q_loads[i].wait()
        part = jnp.dot(normed[...], qw[i], preferred_element_type=F32)
        for t in range(Q_CHUNK // 128):
            at = i * Q_CHUNK + t * 128
            qt[at:at + 128] = part[:, t * 128:(t + 1) * 128].T

    for t in pieces_v:
        send_own(t)
    for t in pieces_v:
        send_two(t)

    def docs_all():
        part = docs_buf.at[pl.ds(0, back)]
        return pltpu.make_async_remote_copy(
            src_ref=part, dst_ref=part, send_sem=doc_sem.at[0], recv_sem=doc_sem.at[1],
            device_id={"cp": me}, device_id_type=MESH,
        )

    for i in range(DOC_AT):
        q_part(i)

    for i in range(5, 8):
        loads[i].wait()
    spread = (iota((shards, rows), 1) // block_rows == iota((shards, rows), 0)).astype(F32)
    owner_row = jnp.broadcast_to(owner_ref[...].astype(F32), (8, shards))
    owner_wide = exact_dot(owner_row, spread)[:1]
    chosen = jnp.broadcast_to(owner_wide, (shards, rows)) == iota((shards, rows), 0).astype(F32)
    chosen = chosen.astype(F32).astype(BF16)
    chosen3[...] = jnp.concatenate([chosen] * 3, axis=1)

    square = (rows, 128)
    lane = iota(square, 1)
    sub = iota(square, 0)
    own_col = jnp.broadcast_to(own_docs.astype(F32), square).T

    docs_all().wait_recv()
    count = jnp.zeros(square, F32)
    for b in range(back + 1):
        window_docs = docs_buf[b].astype(F32)
        if b < back:
            window_docs = jnp.where(me >= back - b, window_docs, -1.0)
        count = count + (jnp.broadcast_to(window_docs, square) < own_col).astype(F32)
    start_row = jnp.broadcast_to(jnp.sum(count, axis=1, keepdims=True), square).T
    within = (lane[:half] + back * rows).astype(F32) - start_row[:half]
    cosine, sine = cos_sin(within * freq_ref[...])

    def rope(u):
        a, b = u[:half], u[half:]
        return jnp.concatenate([a * cosine - b * sine, b * cosine + a * sine], axis=0)

    for t in range(kv_heads // 2):
        u = raw_kt[t]
        u = jnp.concatenate([rope(u[:HEAD_DIM]), rope(u[HEAD_DIM:])], axis=0)
        kbuf[back, t] = u.T.astype(BF16)
    for t in pieces_k:
        send_own(t)
    for t in pieces_k:
        send_two(t)

    for t in pieces_v:
        serve(t, 0)
    for i in range(DOC_AT, n_chunks):
        q_part(i)

    scale = HEAD_DIM ** (-0.5)
    zeros = jnp.zeros((HEAD_DIM, rows), BF16)
    for h in range(heads):
        y = (rope(qt[h * HEAD_DIM:(h + 1) * HEAD_DIM]) * scale).astype(BF16)
        at = (h // per_kv) % 2
        lanes = slice((h % HEADS_STEP) * rows, (h % HEADS_STEP + 1) * rows)
        qz[h // HEADS_STEP, at * HEAD_DIM:(at + 1) * HEAD_DIM, lanes] = y
        qz[h // HEADS_STEP, (1 - at) * HEAD_DIM:(2 - at) * HEAD_DIM, lanes] = zeros

    for b in range(back + 1):
        place = (sub + b * rows).astype(F32)
        allowed = place >= start_row
        if b == back:
            allowed = allowed & (sub <= lane)
        bias[b] = jnp.where(allowed, 0.0, MASKED)

    extra = 1 + 6 * core
    front = (3 - z) // 3
    one = 6 - 4 * front
    three = 2 + 4 * front
    two_ = 12 - one - three

    def odd(slot):
        return slot + 1 - 2 * core

    def serve_all(slot):
        for t in pieces_v + pieces_k:
            serve(t, slot)

    def wait_all(slot):
        for t in pieces_v + pieces_k:
            arrived(t, slot)

    def serve_next_row():
        for t in pieces_k:
            serve(t, 0)

    def before_first():
        serve_next_row()

        @pl.when(z > 1)
        def _():
            serve_all(one)

        wait_all(extra)

    def serve_first():
        @pl.when(z <= 1)
        def _():
            serve_all(one)

    def odd_pair():
        wait_all(odd(one))
        wait_all(odd(two_))

    groups = (
        ((back,), lambda: None, -1, None),
        ((0, extra), before_first, HOOK_0, serve_first),
        ((one, two_), lambda: serve_all(two_), HOOK_1, lambda: serve_all(three)),
        ((odd(one), odd(two_)), odd_pair, -1, None),
        ((three, odd(three)), lambda: wait_all(odd(three)), -1, None),
    )
    two = HEADS_STEP * rows
    head_lane = iota((1, two), 1) // rows
    acc_rows = HEAD_DIM + 16
    for gi, (slots, before, hook_at, hook) in enumerate(groups):
        with jax.named_scope("before%d" % gi):
            before()
        first, last = gi == 0, gi == len(groups) - 1
        nb = len(slots)
        ones_rows = jnp.ones((16, nb * rows), BF16)

        def score(j, s_ref, t_ref, slots=slots, nb=nb):
            a = j // (per_kv // HEADS_STEP)
            kb = jnp.concatenate([kbuf[b, a // 2] for b in slots], axis=0)
            s = jnp.dot(kb, qz[j], preferred_element_type=F32)
            top = None
            for b in range(nb):
                bb = bias[slots[b]]
                sb = s[b * rows:(b + 1) * rows] * LOG2E + jnp.concatenate([bb] * HEADS_STEP, axis=1)
                s_ref[b * rows:(b + 1) * rows] = sb
                part = jnp.max(sb.reshape(rows // 8, 8, two), axis=0)
                top = part if top is None else jnp.maximum(top, part)
            t_ref[...] = top

        def mix(j, s_ref, t_ref, slots=slots, nb=nb, first=first, last=last, ones_rows=ones_rows):
            a = j // (per_kv // HEADS_STEP)
            top = jnp.max(t_ref[...], axis=0, keepdims=True)
            if first:
                old = jnp.zeros((1, two), F32)
                for i in range(HEADS_STEP):
                    old = jnp.where(head_lane == i, sink_ref[HEADS_STEP * j + i] * LOG2E, old)
            else:
                old = m_ref[j][:1]
            new = jnp.maximum(old, top)
            mixed = None
            for b in range(0, nb, 2):
                part = slots[b:b + 2]
                n = len(part) * rows
                weights = jnp.exp2(s_ref[b * rows:b * rows + n] - new).astype(BF16)
                vt = jnp.concatenate([vbuf[i, a] for i in part], axis=1)
                vt = jnp.concatenate([vt, ones_rows[:, :n]], axis=0)
                more = jnp.dot(vt, weights, preferred_element_type=F32)
                mixed = more if mixed is None else mixed + more
            shrink = jnp.exp2(old - new)
            if first:
                acc = mixed + jnp.where(iota((acc_rows, two), 0) >= HEAD_DIM, shrink, 0.0)
            else:
                acc = acc_ref[j] * shrink + mixed
            if last:
                total = acc[HEAD_DIM:HEAD_DIM + 1]
                acc_ref[j] = acc
                lse = (new + jnp.log2(total)) * LN2
                for i in range(HEADS_STEP):
                    lse_ref[pl.ds(HEADS_STEP * j + i, 1), :] = lse[:, i * rows:(i + 1) * rows]
            else:
                acc_ref[j] = acc
                m_ref[j] = jnp.broadcast_to(new, (8, two))

        def two_pairs(i, carry, score=score, mix=mix):
            j = 2 * i
            score(j + 1, s_odd, top_odd)
            mix(j, s_even, top_even)
            score(lax.rem(j + 2, pairs), s_even, top_even)
            mix(j + 1, s_odd, top_odd)
            return carry

        with jax.named_scope("loop%d" % gi):
            score(0, s_even, top_even)
            for j in range(0, pairs, 2):
                if j == hook_at:
                    with jax.named_scope("hook%d" % gi):
                        hook()
                score(j + 1, s_odd, top_odd)
                mix(j, s_even, top_even)
                if j + 2 < pairs:
                    score(j + 2, s_even, top_even)
                mix(j + 1, s_odd, top_odd)

    for c in cnt_copies:
        c.wait_recv()
    cnt = cnt_buf[0]
    for k in range(1, dps):
        cnt = cnt + cnt_buf[k]

    def pieces(v):
        hi = v.astype(BF16)
        rest = v - hi.astype(F32)
        mid = rest.astype(BF16)
        return [hi, mid, (rest - mid.astype(F32)).astype(BF16)]

    wide = block_rows * heads
    lse4 = jnp.concatenate([lse_ref[...]] * block_rows, axis=0)
    lse4 = jnp.where(iota((wide, rows), 1) % block_rows == iota((wide, rows), 0) // heads, lse4, 0.0)
    lse4 = jnp.concatenate(pieces(lse4), axis=1)
    comb_send[:, 0, :] = lax.dot_general(chosen3[...], lse4, NT, preferred_element_type=F32)
    comb_send[:, 1, :] = jnp.broadcast_to(cnt, (shards, rows))
    comb[me] = comb_send[me]

    def lse_send(k, carry):
        pltpu.make_async_remote_copy(
            src_ref=comb_send.at[ahead(k)], dst_ref=comb.at[me],
            send_sem=lse_sem.at[0], recv_sem=lse_sem.at[1],
            device_id={"cp": ahead(k)}, device_id_type=MESH,
        ).start()
        return carry

    lax.fori_loop(1, shards, lse_send, 0, unroll=True)

    for j in range(pairs):
        acc = acc_ref[j]
        out = acc[:HEAD_DIM] * (1.0 / acc[HEAD_DIM:HEAD_DIM + 1])
        for i in range(0, HEADS_STEP, 2):
            both = jnp.concatenate([out[:, i * rows:(i + 1) * rows], out[:, (i + 1) * rows:(i + 2) * rows]], axis=0).T
            at = (j * HEADS_STEP + i) * HEAD_DIM
            att_ref[:, at:at + 128] = both.astype(BF16)
    att_copy = pltpu.make_async_copy(att_ref, att_hbm, load_sem.at[0])
    att_copy.start()
    def lse_all():
        part = comb.at[pl.ds(0, shards - 1)]
        return pltpu.make_async_remote_copy(
            src_ref=part, dst_ref=part, send_sem=lse_sem.at[0], recv_sem=lse_sem.at[1],
            device_id={"cp": me}, device_id_type=MESH,
        )

    lse_all().wait_recv()

    got = comb[:, 0, :].T
    totals = jnp.sum(comb[:, 1, :], axis=0, keepdims=True)
    tw_ref[...] = flags * (float(dps * shards * rows) / totals)
    tw_move = pltpu.make_async_copy(tw_ref, tw_hbm, load_sem.at[2])
    tw_move.start()
    placed = None
    for r in range(block_rows):
        part = jnp.concatenate(pieces(got[r * heads:(r + 1) * heads]), axis=0)
        to = (iota((shards, rows), 1) == iota((shards, rows), 0) * block_rows + r).astype(F32).astype(BF16)
        more = jnp.dot(part, to, preferred_element_type=F32)
        placed = more if placed is None else placed + more
    lse_out_ref[...] = placed[:heads] + placed[heads:2 * heads] + placed[2 * heads:]
    lse_move = pltpu.make_async_copy(lse_out_ref, lse_hbm, load_sem.at[1])
    lse_move.start()

    for c in sends:
        c.wait_send()
    docs_all().wait_send()
    for t in range(4):
        for sem in range(2 * chips):
            slot_copy(t, back, 0, sem, me).wait_send()
    lse_all().wait_send()
    att_copy.wait()
    tw_move.wait()
    lse_move.wait()


def store(att_in, lse_in, tw_in, att_out, lse_out, tw_out, att, lse, tw, in_sem, out_sem):
    parts = 4
    step = att.shape[0] // parts
    moves = [(att_in.at[pl.ds(i * step, step)], att.at[pl.ds(i * step, step)], att_out.at[pl.ds(i * step, step)]) for i in range(parts)]
    moves += [(lse_in, lse, lse_out), (tw_in, tw, tw_out)]
    ins = [pltpu.make_async_copy(a, b, in_sem.at[i]) for i, (a, b, c) in enumerate(moves)]
    outs = [pltpu.make_async_copy(b, c, out_sem.at[i]) for i, (a, b, c) in enumerate(moves)]
    for c in ins:
        c.start()
    for i, c in enumerate(outs):
        ins[i].wait()
        c.start()
    for c in outs:
        c.wait()


def solution(mesh):
    dps, shards = mesh.shape["dp"], mesh.shape["cp"]
    half = HEAD_DIM // 2
    freq_np = np.broadcast_to(ROPE_BASE ** (-np.arange(half).astype(np.float64) / half)[:, None], (half, 128))

    def body(hidden, norm_gain, query_weight, keyval_weight, sink_logits, document_ids, block_owner, loss_mask):
        rows, width = hidden.shape[1:]
        heads = sink_logits.shape[0]
        kv_heads = keyval_weight.shape[1] // (2 * HEAD_DIM)
        qdim = heads * HEAD_DIM
        back = DOC_MOST // rows
        slots = back + 1
        pairs = heads // HEADS_STEP
        widest = 2 * rows
        shape = (rows, width, heads, kv_heads, shards, dps)
        hbm = pl.BlockSpec(memory_space=pltpu.HBM)
        dma = pltpu.SemaphoreType.DMA
        att, lse, tw = pl.pallas_call(
            functools.partial(kernel, shape),
            name="attention_step",
            out_shape=(
                jax.ShapeDtypeStruct((rows, qdim), BF16),
                jax.ShapeDtypeStruct((heads, rows), F32),
                jax.ShapeDtypeStruct((1, rows), F32),
            ),
            in_specs=[hbm] * 9,
            out_specs=(hbm, hbm, hbm),
            scratch_shapes=[
                pltpu.VMEM((width, rows), BF16),
                pltpu.VMEM((width,), F32),
                pltpu.VMEM((width, keyval_weight.shape[1]), BF16),
                pltpu.VMEM((qdim // Q_CHUNK, width, Q_CHUNK), BF16),
                pltpu.VMEM((rows, width), BF16),
                pltpu.VMEM((qdim, rows), F32),
                pltpu.VMEM((pairs, 128, HEADS_STEP * rows), BF16),
                pltpu.VMEM((slots, kv_heads // 2, rows, 128), BF16),
                pltpu.VMEM((slots, kv_heads, HEAD_DIM, rows), BF16),
                pltpu.VMEM((slots, rows, rows), F32),
                pltpu.VMEM((slots, 1, rows), jnp.int32),
                pltpu.VMEM((1, 1, rows), F32),
                pltpu.VMEM((dps, 1, rows), F32),
                pltpu.VMEM((pairs, 8, HEADS_STEP * rows), F32),
                pltpu.VMEM((pairs, HEAD_DIM + 16, HEADS_STEP * rows), F32),
                pltpu.VMEM((heads, rows), F32),
                pltpu.VMEM((shards, 2, rows), F32),
                pltpu.VMEM((shards, 2, rows), F32),
                pltpu.VMEM((widest, HEADS_STEP * rows), F32),
                pltpu.VMEM((widest, HEADS_STEP * rows), F32),
                pltpu.VMEM((8, HEADS_STEP * rows), F32),
                pltpu.VMEM((8, HEADS_STEP * rows), F32),
                pltpu.VMEM((shards, 3 * rows), BF16),
                pltpu.SMEM((heads,), F32),
                pltpu.VMEM((1, shards), jnp.int32),
                pltpu.VMEM((1, rows), jnp.int32),
                pltpu.VMEM((half, 128), F32),
                pltpu.VMEM((rows, qdim), BF16),
                pltpu.VMEM((heads, rows), F32),
                pltpu.VMEM((1, rows), F32),
                dma((8,)), dma((qdim // Q_CHUNK,)),
                dma((2,)),
                dma((4, back)), dma((4, back)),
                dma((dps - 1,)), dma((dps - 1,)),
                dma((2,)),
            ],
            compiler_params=pltpu.CompilerParams(
                collective_id=0, has_side_effects=True, vmem_limit_bytes=58 * 1024 * 1024
            ),
        )(
            hidden[0].T, norm_gain, query_weight, keyval_weight, sink_logits,
            document_ids, block_owner[0], loss_mask,
            jnp.asarray(freq_np, F32),
        )
        results = (att, lse, tw)
        att, lse, tw = pl.pallas_call(
            store,
            name="store_results",
            out_shape=tuple(jax.ShapeDtypeStruct(r.shape, r.dtype) for r in results),
            in_specs=[hbm] * 3,
            out_specs=(hbm,) * 3,
            scratch_shapes=[pltpu.VMEM(r.shape, r.dtype) for r in results] + [dma((6,)), dma((6,))],
            compiler_params=pltpu.CompilerParams(vmem_limit_bytes=58 * 1024 * 1024),
        )(*results)
        return att[None], lse[None], tw

    return jax.shard_map(
        body,
        mesh=mesh,
        in_specs=(
            P("dp", "cp", None), P(), P(), P(), P(), P("dp", "cp"), P("dp", "cp", None), P("dp", "cp"),
        ),
        out_specs=(P("dp", "cp", None), P("dp", None, "cp"), P("dp", "cp")),
        check_vma=False,
    )
```

```python
import functools
import math

import jax
import jax.numpy as jnp
import numpy as np
from jax import lax
from jax.experimental import pallas as pl
from jax.experimental.pallas import tpu as pltpu
from jax.sharding import PartitionSpec as P

MESH = pl.DeviceIdType.MESH
HEAD_DIM = 64
DOC_MOST = 1024
ROPE_BASE = 150000.0
NORM_EPS = 1e-05
MASKED = -1e30
LOG2E = 1.4426950408889634
LN2 = 0.6931471805599453
F32 = jnp.float32
BF16 = jnp.bfloat16
NT = (((1,), (1,)), ((), ()))
Q_CHUNK = 512
HEADS_STEP = 8
DOC_AT = 3
HOOK_0, HOOK_1 = 2, 2


def iota(shape, dim):
    return lax.broadcasted_iota(jnp.int32, shape, dim)


def exact_dot(a, b, dims=(((1,), (0,)), ((), ()))):
    return lax.dot_general(a, b, dims, precision=lax.Precision.HIGHEST, preferred_element_type=F32)


def cos_sin(angle):
    k = jnp.floor(angle * (2.0 / math.pi) + 0.5)
    r = ((angle - k * 1.5703125) - k * 4.837512969970703125e-4) - k * 7.549789954891882e-8
    z = r * r
    s = ((-1.9515295891e-4 * z + 8.3321608736e-3) * z - 1.6666654611e-1) * z * r + r
    c = ((2.443315711809948e-5 * z - 1.388731625493765e-3) * z + 4.166664568298827e-2) * z * z - 0.5 * z + 1.0
    q = k.astype(jnp.int32) & 3
    odd = (q & 1) == 1
    cosine = jnp.where(odd, s, c)
    sine = jnp.where(odd, c, s)
    cosine = jnp.where((q == 1) | (q == 2), -cosine, cosine)
    sine = jnp.where(q >= 2, -sine, sine)
    return cosine, sine


def kernel(
    shape,
    hidden_hbm, gain_hbm, qw_hbm, kvw_hbm, sink_hbm, docs_hbm, owner_hbm, mask_hbm, freq_hbm,
    att_hbm, lse_hbm, tw_hbm,
    hid, gain, kvw, qw, normed, qt, qz, kbuf, vbuf, bias,
    docs_buf, cnt_send, cnt_buf, m_ref, acc_ref, lse_ref, comb_send, comb, s_even, s_odd, top_even, top_odd,
    chosen3, sink_ref, owner_ref, mask_ref, freq_ref, att_ref, lse_out_ref, tw_ref,
    load_sem, qw_sem,
    doc_sem, kv_ssem, kv_rsem, cnt_ssem, cnt_rsem, lse_sem,
):
    rows, width, heads, kv_heads, shards, dps = shape
    back = DOC_MOST // rows
    per_kv = heads // kv_heads
    block_rows = rows // shards
    me = lax.axis_index("cp")
    my_dp = lax.axis_index("dp")
    qdim = heads * HEAD_DIM
    n_chunks = qdim // Q_CHUNK
    pairs = heads // HEADS_STEP
    half = HEAD_DIM // 2

    def ahead(k):
        return lax.rem(me + k, shards)

    loads = [
        pltpu.make_async_copy(hidden_hbm, hid, load_sem.at[0]),
        pltpu.make_async_copy(gain_hbm, gain, load_sem.at[1]),
        pltpu.make_async_copy(docs_hbm, docs_buf.at[back], load_sem.at[2]),
        pltpu.make_async_copy(mask_hbm, mask_ref, load_sem.at[3]),
        pltpu.make_async_copy(kvw_hbm, kvw, load_sem.at[4]),
        pltpu.make_async_copy(freq_hbm, freq_ref, load_sem.at[5]),
        pltpu.make_async_copy(sink_hbm, sink_ref, load_sem.at[6]),
        pltpu.make_async_copy(owner_hbm, owner_ref, load_sem.at[7]),
    ]
    for c in loads:
        c.start()

    barrier = pltpu.get_barrier_semaphore()

    for k in range(1, back + 1):
        for at in (k, shards - k):
            pl.semaphore_signal(barrier, inc=1, device_id={"cp": ahead(at)}, device_id_type=MESH)
    for k in range(1, dps):
        pl.semaphore_signal(
            barrier, inc=1, device_id={"dp": lax.rem(my_dp + k, dps)}, device_id_type=MESH
        )

    loads[0].wait()
    loads[1].wait()
    q_loads = [
        pltpu.make_async_copy(qw_hbm.at[:, pl.ds(i * Q_CHUNK, Q_CHUNK)], qw.at[i], qw_sem.at[i])
        for i in range(n_chunks)
    ]
    for c in q_loads:
        c.start()
    loads[2].wait()
    loads[3].wait()
    own_docs = docs_buf[back]
    flags = mask_ref[...].astype(F32)
    cnt_row = jnp.broadcast_to(jnp.sum(flags, axis=1, keepdims=True), (1, rows))
    cnt_send[0] = cnt_row
    cnt_buf[0] = cnt_row
    x = hid[...].T.astype(F32)
    inv = lax.rsqrt(jnp.sum(x * x, axis=1, keepdims=True) * (1.0 / width) + NORM_EPS)
    normed[...] = (x * inv * gain[...].reshape(1, width)).astype(BF16)

    pl.semaphore_wait(barrier, 2 * back + dps - 1)

    sends = []

    def send(src, dst, ssem, rsem, device, keep=True):
        c = pltpu.make_async_remote_copy(
            src_ref=src, dst_ref=dst, send_sem=ssem, recv_sem=rsem,
            device_id=device, device_id_type=MESH,
        )
        c.start()
        if keep:
            sends.append(c)
        return c

    for k in range(1, back + 1):
        send(docs_buf.at[back], docs_buf.at[back - k], doc_sem.at[0], doc_sem.at[1], {"cp": ahead(k)}, False)
    cnt_copies = []
    for k in range(1, dps):
        cnt_copies.append(send(
            cnt_send.at[0], cnt_buf.at[k], cnt_ssem.at[k - 1], cnt_rsem.at[k - 1],
            {"dp": lax.rem(my_dp + k, dps)},
        ))

    core = lax.rem(me, 2)
    chips = back // 2
    z = lax.rem(me // 2, chips)
    corner = me - 2 * z
    pieces_v, pieces_k = (0, 1), (2, 3)

    def piece(t, slot):
        if t < 2:
            return vbuf.at[slot, pl.ds(t * (kv_heads // 2), kv_heads // 2)]
        return kbuf.at[slot, t - 2]

    def whole(kind, part):
        buf = (vbuf, kbuf)[kind].at[part]
        return pltpu.make_async_remote_copy(
            src_ref=buf, dst_ref=buf, send_sem=kv_ssem.at[kind],
            recv_sem=kv_rsem.at[kind, 0 if isinstance(part, slice) else part],
            device_id={"cp": me}, device_id_type=MESH,
        )

    def slot_copy(t, src, dst, device):
        second = isinstance(dst, int) and dst == 0 and t % 2 == 1
        return pltpu.make_async_remote_copy(
            src_ref=piece(t, src), dst_ref=piece(t, dst), send_sem=kv_ssem.at[t // 2],
            recv_sem=kv_rsem.at[t // 2, back if second else dst], device_id={"cp": device}, device_id_type=MESH,
        )

    def row_copy(t, k, src):
        return slot_copy(t, src, back - 2 * k, corner + 2 * lax.rem(z + k, chips))

    def next_row_copy(t):
        return slot_copy(t, back, 0, ahead(back))

    def partner_copy(t, src, dst):
        return slot_copy(t, src, dst, me + 1 - 2 * core)

    def send_own(t):
        @pl.when(core == 0)
        def _():
            partner_copy(t, back, back - 1).start()

        next_row_copy(t).start()
        @pl.when(z == 0)
        def _():
            row_copy(t, 3, back).start()

        @pl.when(z < chips - 1)
        def _():
            row_copy(t, 1, back).start()

    def send_two(t):
        @pl.when(z == 1)
        def _():
            slot_copy(t, back, back - 6, ahead(6)).start()

        slot_copy(t, back, back // 2, ahead(back // 2)).start()

    def serve(t):
        slot_copy(t, 0, 0, me).wait_recv()

        @pl.when(z > 1)
        def _():
            row_copy(t, 3, 0).start()

        @pl.when(z == chips - 1)
        def _():
            row_copy(t, 1, 0).start()

        @pl.when(core == 1)
        def _():
            partner_copy(t, 0, 1).start()

    loads[4].wait()
    kv = jnp.dot(normed[...], kvw[...], preferred_element_type=F32)
    kv_width = kv_heads * HEAD_DIM
    raw_kt = []
    for t in range(kv_heads // 2):
        v_t = kv[:, kv_width + t * 128:kv_width + (t + 1) * 128].T.astype(BF16)
        vbuf[back, 2 * t] = v_t[:HEAD_DIM]
        vbuf[back, 2 * t + 1] = v_t[HEAD_DIM:]
        raw_kt.append(kv[:, t * 128:(t + 1) * 128].T)

    def q_part(i):
        q_loads[i].wait()
        part = jnp.dot(normed[...], qw[i], preferred_element_type=F32)
        for t in range(Q_CHUNK // 128):
            at = i * Q_CHUNK + t * 128
            qt[at:at + 128] = part[:, t * 128:(t + 1) * 128].T

    for t in pieces_v:
        send_own(t)
    for t in pieces_v:
        send_two(t)

    def docs_all():
        part = docs_buf.at[pl.ds(0, back)]
        return pltpu.make_async_remote_copy(
            src_ref=part, dst_ref=part, send_sem=doc_sem.at[0], recv_sem=doc_sem.at[1],
            device_id={"cp": me}, device_id_type=MESH,
        )

    for i in range(DOC_AT):
        q_part(i)

    for i in range(5, 8):
        loads[i].wait()
    spread = (iota((shards, rows), 1) // block_rows == iota((shards, rows), 0)).astype(F32)
    owner_row = jnp.broadcast_to(owner_ref[...].astype(F32), (8, shards))
    owner_wide = exact_dot(owner_row, spread)[:1]
    chosen = jnp.broadcast_to(owner_wide, (shards, rows)) == iota((shards, rows), 0).astype(F32)
    chosen = chosen.astype(F32).astype(BF16)
    chosen3[...] = jnp.concatenate([chosen] * 3, axis=1)

    square = (rows, 128)
    lane = iota(square, 1)
    sub = iota(square, 0)
    own_col = jnp.broadcast_to(own_docs.astype(F32), square).T

    docs_all().wait_recv()
    count = jnp.zeros(square, F32)
    for b in range(back + 1):
        window_docs = docs_buf[b].astype(F32)
        if b < back:
            window_docs = jnp.where(me >= back - b, window_docs, -1.0)
        count = count + (jnp.broadcast_to(window_docs, square) < own_col).astype(F32)
    start_row = jnp.broadcast_to(jnp.sum(count, axis=1, keepdims=True), square).T
    within = (lane[:half] + back * rows).astype(F32) - start_row[:half]
    cosine, sine = cos_sin(within * freq_ref[...])

    def rope(u):
        a, b = u[:half], u[half:]
        return jnp.concatenate([a * cosine - b * sine, b * cosine + a * sine], axis=0)

    for t in range(kv_heads // 2):
        u = raw_kt[t]
        u = jnp.concatenate([rope(u[:HEAD_DIM]), rope(u[HEAD_DIM:])], axis=0)
        kbuf[back, t] = u.T.astype(BF16)
    for t in pieces_k:
        send_own(t)
    for t in pieces_k:
        send_two(t)

    for t in pieces_v:
        serve(t)
    for i in range(DOC_AT, n_chunks):
        q_part(i)

    scale = HEAD_DIM ** (-0.5)
    zeros = jnp.zeros((HEAD_DIM, rows), BF16)
    for h in range(heads):
        y = (rope(qt[h * HEAD_DIM:(h + 1) * HEAD_DIM]) * scale).astype(BF16)
        at = (h // per_kv) % 2
        lanes = slice((h % HEADS_STEP) * rows, (h % HEADS_STEP + 1) * rows)
        qz[h // HEADS_STEP, at * HEAD_DIM:(at + 1) * HEAD_DIM, lanes] = y
        qz[h // HEADS_STEP, (1 - at) * HEAD_DIM:(2 - at) * HEAD_DIM, lanes] = zeros

    for b in range(back + 1):
        place = (sub + b * rows).astype(F32)
        allowed = place >= start_row
        if b == back:
            allowed = allowed & (sub <= lane)
        bias[b] = jnp.where(allowed, 0.0, MASKED)

    extra = 1 + 6 * core
    front = (3 - z) // 3
    one = 6 - 4 * front
    three = 2 + 4 * front
    two_ = 12 - one - three

    def odd(slot):
        return slot + 1 - 2 * core

    def serve_all(slot):
        for kind in range(2):
            whole(kind, slot).wait_recv()
            for t in (2 * kind, 2 * kind + 1):
                partner_copy(t, slot, slot - 1 + 2 * core).start()

    def wait_all(slot):
        for kind in range(2):
            whole(kind, slot).wait_recv()

    def serve_next_row():
        for t in pieces_k:
            serve(t)

    def before_first():
        serve_next_row()

        @pl.when(z > 1)
        def _():
            serve_all(one)

        wait_all(extra)

    def serve_first():
        @pl.when(z <= 1)
        def _():
            serve_all(one)

    def odd_pair():
        wait_all(odd(one))
        wait_all(odd(two_))

    groups = (
        ((back,), lambda: None, -1, None),
        ((0, extra), before_first, HOOK_0, serve_first),
        ((one, two_), lambda: serve_all(two_), HOOK_1, lambda: serve_all(three)),
        ((odd(one), odd(two_)), odd_pair, -1, None),
        ((three, odd(three)), lambda: wait_all(odd(three)), -1, None),
    )
    two = HEADS_STEP * rows
    head_lane = iota((1, two), 1) // rows
    acc_rows = HEAD_DIM + 16
    for gi, (slots, before, hook_at, hook) in enumerate(groups):
        with jax.named_scope("before%d" % gi):
            before()
        first, last = gi == 0, gi == len(groups) - 1
        nb = len(slots)
        ones_rows = jnp.ones((16, nb * rows), BF16)

        def score(j, s_ref, t_ref, slots=slots, nb=nb):
            a = j // (per_kv // HEADS_STEP)
            kb = jnp.concatenate([kbuf[b, a // 2] for b in slots], axis=0)
            s = jnp.dot(kb, qz[j], preferred_element_type=F32)
            top = None
            for b in range(nb):
                bb = bias[slots[b]]
                sb = s[b * rows:(b + 1) * rows] * LOG2E + jnp.concatenate([bb] * HEADS_STEP, axis=1)
                s_ref[b * rows:(b + 1) * rows] = sb
                part = jnp.max(sb.reshape(rows // 8, 8, two), axis=0)
                top = part if top is None else jnp.maximum(top, part)
            t_ref[...] = top

        def mix(j, s_ref, t_ref, slots=slots, nb=nb, first=first, last=last, ones_rows=ones_rows):
            a = j // (per_kv // HEADS_STEP)
            top = jnp.max(t_ref[...], axis=0, keepdims=True)
            if first:
                old = jnp.zeros((1, two), F32)
                for i in range(HEADS_STEP):
                    old = jnp.where(head_lane == i, sink_ref[HEADS_STEP * j + i] * LOG2E, old)
            else:
                old = m_ref[j][:1]
            new = jnp.maximum(old, top)
            mixed = None
            for b in range(0, nb, 2):
                part = slots[b:b + 2]
                n = len(part) * rows
                weights = jnp.exp2(s_ref[b * rows:b * rows + n] - new).astype(BF16)
                vt = jnp.concatenate([vbuf[i, a] for i in part], axis=1)
                vt = jnp.concatenate([vt, ones_rows[:, :n]], axis=0)
                more = jnp.dot(vt, weights, preferred_element_type=F32)
                mixed = more if mixed is None else mixed + more
            shrink = jnp.exp2(old - new)
            if first:
                acc = mixed + jnp.where(iota((acc_rows, two), 0) >= HEAD_DIM, shrink, 0.0)
            else:
                acc = acc_ref[j] * shrink + mixed
            if last:
                total = acc[HEAD_DIM:HEAD_DIM + 1]
                acc_ref[j] = acc
                lse = (new + jnp.log2(total)) * LN2
                for i in range(HEADS_STEP):
                    lse_ref[pl.ds(HEADS_STEP * j + i, 1), :] = lse[:, i * rows:(i + 1) * rows]
            else:
                acc_ref[j] = acc
                m_ref[j] = jnp.broadcast_to(new, (8, two))

        def two_pairs(i, carry, score=score, mix=mix):
            j = 2 * i
            score(j + 1, s_odd, top_odd)
            mix(j, s_even, top_even)
            score(lax.rem(j + 2, pairs), s_even, top_even)
            mix(j + 1, s_odd, top_odd)
            return carry

        with jax.named_scope("loop%d" % gi):
            score(0, s_even, top_even)
            for j in range(0, pairs, 2):
                if j == hook_at:
                    with jax.named_scope("hook%d" % gi):
                        hook()
                score(j + 1, s_odd, top_odd)
                mix(j, s_even, top_even)
                if j + 2 < pairs:
                    score(j + 2, s_even, top_even)
                mix(j + 1, s_odd, top_odd)

    for c in cnt_copies:
        c.wait_recv()
    cnt = cnt_buf[0]
    for k in range(1, dps):
        cnt = cnt + cnt_buf[k]

    def pieces(v):
        hi = v.astype(BF16)
        rest = v - hi.astype(F32)
        mid = rest.astype(BF16)
        return [hi, mid, (rest - mid.astype(F32)).astype(BF16)]

    wide = block_rows * heads
    lse4 = jnp.concatenate([lse_ref[...]] * block_rows, axis=0)
    lse4 = jnp.where(iota((wide, rows), 1) % block_rows == iota((wide, rows), 0) // heads, lse4, 0.0)
    lse4 = jnp.concatenate(pieces(lse4), axis=1)
    comb_send[:, 0, :] = lax.dot_general(chosen3[...], lse4, NT, preferred_element_type=F32)
    comb_send[:, 1, :] = jnp.broadcast_to(cnt, (shards, rows))
    comb[me] = comb_send[me]

    def lse_send(k, carry):
        pltpu.make_async_remote_copy(
            src_ref=comb_send.at[ahead(k)], dst_ref=comb.at[me],
            send_sem=lse_sem.at[0], recv_sem=lse_sem.at[1],
            device_id={"cp": ahead(k)}, device_id_type=MESH,
        ).start()
        return carry

    lax.fori_loop(1, shards, lse_send, 0, unroll=True)

    for j in range(pairs):
        acc = acc_ref[j]
        out = acc[:HEAD_DIM] * (1.0 / acc[HEAD_DIM:HEAD_DIM + 1])
        for i in range(0, HEADS_STEP, 2):
            both = jnp.concatenate([out[:, i * rows:(i + 1) * rows], out[:, (i + 1) * rows:(i + 2) * rows]], axis=0).T
            at = (j * HEADS_STEP + i) * HEAD_DIM
            att_ref[:, at:at + 128] = both.astype(BF16)
    att_copy = pltpu.make_async_copy(att_ref, att_hbm, load_sem.at[0])
    att_copy.start()
    def lse_all():
        part = comb.at[pl.ds(0, shards - 1)]
        return pltpu.make_async_remote_copy(
            src_ref=part, dst_ref=part, send_sem=lse_sem.at[0], recv_sem=lse_sem.at[1],
            device_id={"cp": me}, device_id_type=MESH,
        )

    lse_all().wait_recv()

    got = comb[:, 0, :].T
    totals = jnp.sum(comb[:, 1, :], axis=0, keepdims=True)
    tw_ref[...] = flags * (float(dps * shards * rows) / totals)
    tw_move = pltpu.make_async_copy(tw_ref, tw_hbm, load_sem.at[2])
    tw_move.start()
    placed = None
    for r in range(block_rows):
        part = jnp.concatenate(pieces(got[r * heads:(r + 1) * heads]), axis=0)
        to = (iota((shards, rows), 1) == iota((shards, rows), 0) * block_rows + r).astype(F32).astype(BF16)
        more = jnp.dot(part, to, preferred_element_type=F32)
        placed = more if placed is None else placed + more
    lse_out_ref[...] = placed[:heads] + placed[heads:2 * heads] + placed[2 * heads:]
    lse_move = pltpu.make_async_copy(lse_out_ref, lse_hbm, load_sem.at[1])
    lse_move.start()

    for c in sends:
        c.wait_send()
    docs_all().wait_send()
    for kind in range(2):
        whole(kind, slice(0, back)).wait_send()
    lse_all().wait_send()
    att_copy.wait()
    tw_move.wait()
    lse_move.wait()


def store(att_in, lse_in, tw_in, att_out, lse_out, tw_out, att, lse, tw, in_sem, out_sem):
    parts = 4
    step = att.shape[0] // parts
    moves = [(att_in.at[pl.ds(i * step, step)], att.at[pl.ds(i * step, step)], att_out.at[pl.ds(i * step, step)]) for i in range(parts)]
    moves += [(lse_in, lse, lse_out), (tw_in, tw, tw_out)]
    ins = [pltpu.make_async_copy(a, b, in_sem.at[i]) for i, (a, b, c) in enumerate(moves)]
    outs = [pltpu.make_async_copy(b, c, out_sem.at[i]) for i, (a, b, c) in enumerate(moves)]
    for c in ins:
        c.start()
    for i, c in enumerate(outs):
        ins[i].wait()
        c.start()
    for c in outs:
        c.wait()


def solution(mesh):
    dps, shards = mesh.shape["dp"], mesh.shape["cp"]
    half = HEAD_DIM // 2
    freq_np = np.broadcast_to(ROPE_BASE ** (-np.arange(half).astype(np.float64) / half)[:, None], (half, 128))

    def body(hidden, norm_gain, query_weight, keyval_weight, sink_logits, document_ids, block_owner, loss_mask):
        rows, width = hidden.shape[1:]
        heads = sink_logits.shape[0]
        kv_heads = keyval_weight.shape[1] // (2 * HEAD_DIM)
        qdim = heads * HEAD_DIM
        back = DOC_MOST // rows
        slots = back + 1
        pairs = heads // HEADS_STEP
        widest = 2 * rows
        shape = (rows, width, heads, kv_heads, shards, dps)
        hbm = pl.BlockSpec(memory_space=pltpu.HBM)
        dma = pltpu.SemaphoreType.DMA
        att, lse, tw = pl.pallas_call(
            functools.partial(kernel, shape),
            name="attention_step",
            out_shape=(
                jax.ShapeDtypeStruct((rows, qdim), BF16),
                jax.ShapeDtypeStruct((heads, rows), F32),
                jax.ShapeDtypeStruct((1, rows), F32),
            ),
            in_specs=[hbm] * 9,
            out_specs=(hbm, hbm, hbm),
            scratch_shapes=[
                pltpu.VMEM((width, rows), BF16),
                pltpu.VMEM((width,), F32),
                pltpu.VMEM((width, keyval_weight.shape[1]), BF16),
                pltpu.VMEM((qdim // Q_CHUNK, width, Q_CHUNK), BF16),
                pltpu.VMEM((rows, width), BF16),
                pltpu.VMEM((qdim, rows), F32),
                pltpu.VMEM((pairs, 128, HEADS_STEP * rows), BF16),
                pltpu.VMEM((slots, kv_heads // 2, rows, 128), BF16),
                pltpu.VMEM((slots, kv_heads, HEAD_DIM, rows), BF16),
                pltpu.VMEM((slots, rows, rows), F32),
                pltpu.VMEM((slots, 1, rows), jnp.int32),
                pltpu.VMEM((1, 1, rows), F32),
                pltpu.VMEM((dps, 1, rows), F32),
                pltpu.VMEM((pairs, 8, HEADS_STEP * rows), F32),
                pltpu.VMEM((pairs, HEAD_DIM + 16, HEADS_STEP * rows), F32),
                pltpu.VMEM((heads, rows), F32),
                pltpu.VMEM((shards, 2, rows), F32),
                pltpu.VMEM((shards, 2, rows), F32),
                pltpu.VMEM((widest, HEADS_STEP * rows), F32),
                pltpu.VMEM((widest, HEADS_STEP * rows), F32),
                pltpu.VMEM((8, HEADS_STEP * rows), F32),
                pltpu.VMEM((8, HEADS_STEP * rows), F32),
                pltpu.VMEM((shards, 3 * rows), BF16),
                pltpu.SMEM((heads,), F32),
                pltpu.VMEM((1, shards), jnp.int32),
                pltpu.VMEM((1, rows), jnp.int32),
                pltpu.VMEM((half, 128), F32),
                pltpu.VMEM((rows, qdim), BF16),
                pltpu.VMEM((heads, rows), F32),
                pltpu.VMEM((1, rows), F32),
                dma((8,)), dma((qdim // Q_CHUNK,)),
                dma((2,)),
                dma((2,)), dma((2, back + 1)),
                dma((dps - 1,)), dma((dps - 1,)),
                dma((2,)),
            ],
            compiler_params=pltpu.CompilerParams(
                collective_id=0, has_side_effects=True, vmem_limit_bytes=58 * 1024 * 1024
            ),
        )(
            hidden[0].T, norm_gain, query_weight, keyval_weight, sink_logits,
            document_ids, block_owner[0], loss_mask,
            jnp.asarray(freq_np, F32),
        )
        results = (att, lse, tw)
        att, lse, tw = pl.pallas_call(
            store,
            name="store_results",
            out_shape=tuple(jax.ShapeDtypeStruct(r.shape, r.dtype) for r in results),
            in_specs=[hbm] * 3,
            out_specs=(hbm,) * 3,
            scratch_shapes=[pltpu.VMEM(r.shape, r.dtype) for r in results] + [dma((6,)), dma((6,))],
            compiler_params=pltpu.CompilerParams(vmem_limit_bytes=58 * 1024 * 1024),
        )(*results)
        return att[None], lse[None], tw

    return jax.shard_map(
        body,
        mesh=mesh,
        in_specs=(
            P("dp", "cp", None), P(), P(), P(), P(), P("dp", "cp"), P("dp", "cp", None), P("dp", "cp"),
        ),
        out_specs=(P("dp", "cp", None), P("dp", None, "cp"), P("dp", "cp")),
        check_vma=False,
    )
```
